32 devices in a mesh: rep: 1, r: 4 (over z), s: 8 (over x, y, core).
Axes of the slice: x: 2, y: 2, z: 4, core: 2. Of those that a mesh axis runs over, the one named last changes fastest.
Arguments:
- x: bfloat16 [32, 4096, 512], P(('rep', 'r', 's'))
- dy: bfloat16 [32, 4096, 512], P(('rep', 'r', 's'))
- w_gate: bfloat16 [2, 512, 1664], P(None, 's')
- w_up: bfloat16 [2, 512, 1664], P(None, 's')
- w_down: bfloat16 [2, 1664, 512], P(None, 's')
- m_w_gate: float32 [2, 512, 1664], P(None, 's')
- m_w_up: float32 [2, 512, 1664], P(None, 's')
- m_w_down: float32 [2, 1664, 512], P(None, 's')
- v_w_gate: float32 [2, 512, 1664], P(None, 's')
- v_w_up: float32 [2, 512, 1664], P(None, 's')
- v_w_down: float32 [2, 1664, 512], P(None, 's')
Outputs:
- output 1: bfloat16 [2, 512, 1664], P('rep', 's')
- output 2: bfloat16 [2, 512, 1664], P('rep', 's')
- output 3: bfloat16 [2, 1664, 512], P('rep', 's')
- output 4: float32 [2, 512, 1664], P('rep', 's')
- output 5: float32 [2, 512, 1664], P('rep', 's')
- output 6: float32 [2, 1664, 512], P('rep', 's')
- output 7: float32 [2, 512, 1664], P('rep', 's')
- output 8: float32 [2, 512, 1664], P('rep', 's')
- output 9: float32 [2, 1664, 512], P('rep', 's')
All inputs are finite; a program needn't handle non-finite values.
Results may differ from the reference program's by a relative error of at most 0.02.
Values are sent between devices in bfloat16 or wider.
A program may use at most 2 GiB of HBM per device.

```python
import jax
import jax.numpy as jnp
from jax import lax

SEQUENCES = 32
TOKENS = 4096
D = 512
FF = 1664
LAYERS = 2
NAMES = ("w_gate", "w_up", "w_down")
SHAPES = {"w_gate": (LAYERS, D, FF), "w_up": (LAYERS, D, FF), "w_down": (LAYERS, FF, D)}


def bump(key, n, height):
    away = (jnp.arange(n, dtype=jnp.int32) - jax.random.randint(key, (), 0, n, jnp.int32)) % n
    return jnp.where(away < n // 8, height, 1.0)


def together(key, own, strength):
    shared = jax.random.normal(key, own.shape[1:], jnp.float32)
    return (own + strength * shared) * lax.rsqrt(1 + strength * strength)


def setup_inputs(seed: int = 0, part: int = 0) -> dict:
    kx, kdy, ka, kb, kz, kf, kh, kl, *keys = jax.random.split(jax.random.key(seed), 8 + 3 * len(NAMES))
    kx, kdy, ka, kb = (jax.random.fold_in(k, part) for k in (kx, kdy, ka, kb))
    kw, km, kv = (keys[i::3] for i in range(3))
    shape = (SEQUENCES, TOKENS, D)
    much_x, much_dy = jax.random.uniform(kz, (2,), jnp.float32, 0.0, 1.0)
    loud = 2.0 ** jax.random.uniform(jax.random.fold_in(kz, 1), (), jnp.float32, -1.0, 2.0)
    layers = 2.0 ** jax.random.uniform(kl, (LAYERS, 1, 1), jnp.float32, -1.0, 1.0)
    x = together(ka, jax.random.normal(kx, shape, jnp.float32), much_x) * bump(kf, D, 4.0)
    dy = together(kb, jax.random.normal(kdy, shape, jnp.float32), much_dy)
    drawn = {"x": x.astype(jnp.bfloat16), "dy": (loud * dy * (SEQUENCES * TOKENS) ** -0.5).astype(jnp.bfloat16)}
    for key, name in zip(kw, NAMES, strict=True):
        w = jax.random.normal(key, SHAPES[name], jnp.float32) * SHAPES[name][1] ** -0.5
        drawn[name] = (w * {"w_gate": 1.0, "w_up": bump(kh, FF, 4.0), "w_down": layers}[name]).astype(jnp.bfloat16)
    for key, name in zip(km, NAMES, strict=True):
        drawn[f"m_{name}"] = 0.1 * jax.random.normal(key, SHAPES[name], jnp.float32)
    for key, name in zip(kv, NAMES, strict=True):
        drawn[f"v_{name}"] = jax.random.uniform(key, SHAPES[name], jnp.float32, 0.005, 0.015)
    return drawn


def matmul(a, w):
    return jnp.dot(a, w, preferred_element_type=jnp.float32).astype(jnp.bfloat16)


def normed(h):
    wide = h.astype(jnp.float32)
    scale = lax.rsqrt(jnp.mean(wide**2, -1, keepdims=True) + 1e-6)
    return (wide * scale).astype(jnp.bfloat16)


def layer(h, w):
    a = normed(h)
    gate = jnp.dot(a, w["w_gate"], preferred_element_type=jnp.float32)
    up = jnp.dot(a, w["w_up"], preferred_element_type=jnp.float32)
    return h + matmul((jax.nn.silu(gate) * up).astype(jnp.bfloat16), w["w_down"])


def adamw(w, m, v, g):
    m = 0.9 * m + 0.1 * g
    v = 0.95 * v + 0.05 * g * g
    step = m * lax.rsqrt(v + 1e-8) + 0.1 * w
    return (w - 0.02 * step).astype(jnp.bfloat16), m, v


def stack(weights, h):
    return lax.scan(lambda h, w: (layer(h, w), None), h, weights)[0]


def reference(x, dy, w_gate, w_up, w_down, m_w_gate, m_w_up, m_w_down, v_w_gate, v_w_up, v_w_down):
    weights = dict(zip(NAMES, (w_gate, w_up, w_down), strict=True))

    def take(so_far, sequence):
        h, by_y = sequence
        _, back = jax.vjp(lambda w: stack(w, h), weights)
        return jax.tree.map(lambda total, term: total + term.astype(jnp.float32), so_far, back(by_y)[0]), None

    none_yet = {name: jnp.zeros(w.shape, jnp.float32) for name, w in weights.items()}
    by_weights, _ = lax.scan(take, none_yet, (x, dy))
    gradients = [by_weights[name].astype(jnp.bfloat16).astype(jnp.float32) for name in NAMES]
    new = [
        adamw(w.astype(jnp.float32), m, v, g)
        for w, m, v, g in zip((w_gate, w_up, w_down), (m_w_gate, m_w_up, m_w_down), (v_w_gate, v_w_up, v_w_down), gradients, strict=True)
    ]
    return tuple(one[which] for which in range(3) for one in new)
```

```python
import functools

import jax
import jax.numpy as jnp
from jax import lax
from jax.experimental import pallas as pl
from jax.experimental.pallas import tpu as pltpu
from jax.sharding import PartitionSpec as P

F32, BF16 = jnp.float32, jnp.bfloat16
D, FF, TOK = 512, 1664, 4096
TILE = 512
TILES = TOK // TILE
CHUNKS = ((0, 512), (512, 512), (1024, 512), (1536, 128))
VMEM_LIMIT = 66_000_000
ANY = pl.BlockSpec(memory_space=pl.ANY)
WHOLE = pl.BlockSpec(memory_space=pltpu.VMEM)


def dot(a, b):
    return jnp.dot(a, b, preferred_element_type=F32)


def dot_nt(a, b):
    return lax.dot_general(a, b, (((1,), (1,)), ((), ())), preferred_element_type=F32)


def norm(h):
    wide = h.astype(F32)
    scale = lax.rsqrt(jnp.mean(wide * wide, -1, keepdims=True) + 1e-6)
    return wide, scale


def gated(g):
    sig = 0.5 + 0.5 * jnp.tanh(0.5 * g)
    return sig, g * sig


def rows(n):
    return pl.BlockSpec((TILE, n), lambda i: (i, 0))


class Place:
    def __init__(self):
        s, z = lax.axis_index("s"), lax.axis_index("r")
        self.s, self.z = s, z
        self.x, self.y, self.c = s // 4, (s // 2) % 2, s % 2
        x, y, c = self.x, self.y, self.c
        self.partner = x * 4 + y * 2 + (1 - c)
        self.nx = (1 - x) * 4 + y * 2 + c
        self.ny = x * 4 + (1 - y) * 2 + c
        self.diag = (1 - x) * 4 + (1 - y) * 2 + c

    def at(self, s, z=None):
        return (0, self.z if z is None else z, s)


def copy_to(src, dst, send, recv, device):
    return pltpu.make_async_remote_copy(
        src_ref=src, dst_ref=dst, send_sem=send, recv_sem=recv, device_id=device, device_id_type=pl.DeviceIdType.MESH
    )


def signal(barrier, device):
    pl.semaphore_signal(barrier, inc=1, device_id=device, device_id_type=pl.DeviceIdType.MESH)


def gather_kernel(*refs):
    own, out = refs[:6], refs[6:12]
    send, recv, local = refs[12:15]
    p = Place()
    barrier = pltpu.get_barrier_semaphore()
    for n in (p.partner, p.nx, p.ny):
        signal(barrier, p.at(n))
    pl.semaphore_wait(barrier, 3)
    pending = []

    def go(i, k, src, slot, device):
        cp = copy_to(src, out[i].at[slot], send.at[i, k], recv.at[i, k], p.at(device))
        cp.start()
        return cp

    first = []
    for i in range(6):
        keep = pltpu.make_async_copy(own[i], out[i].at[p.s], local.at[i])
        keep.start()
        pending.append(keep)
        first.append((go(i, 0, own[i], p.s, p.nx), go(i, 1, own[i], p.s, p.ny), go(i, 2, own[i], p.s, p.partner)))
    for i in range(6):
        cx, cy, cp = first[i]
        cx.wait_recv()
        fx = go(i, 3, out[i].at[p.nx], p.nx, p.partner)
        if i % 2 == 0:
            dg = go(i, 5, out[i].at[p.nx], p.nx, p.ny)
        cy.wait_recv()
        fy = go(i, 4, out[i].at[p.ny], p.ny, p.partner)
        if i % 2 == 1:
            dg = go(i, 5, out[i].at[p.ny], p.ny, p.nx)
        first[i] = (cx, cy, cp, fx, fy, dg)
    for i in range(6):
        cx, cy, cp, fx, fy, dg = first[i]
        dg.wait_recv()
        fd = go(i, 6, out[i].at[p.diag], p.diag, p.partner)
        first[i] = (cx, cy, cp, fx, fy, dg, fd)
    for i in range(6):
        cx, cy, cp, fx, fy, dg, fd = first[i]
        for w in (cp, fx, fy, fd):
            w.wait_recv()
        for w in first[i]:
            w.wait_send()
    for keep in pending:
        keep.wait()


def gather(weights):
    own = [w[l] for l in range(2) for w in weights]
    out = pl.pallas_call(
        gather_kernel,
        out_shape=[jax.ShapeDtypeStruct((8,) + o.shape, BF16) for o in own],
        in_specs=[ANY] * 6,
        out_specs=[ANY] * 6,
        scratch_shapes=[pltpu.SemaphoreType.DMA((6, 7)), pltpu.SemaphoreType.DMA((6, 7)), pltpu.SemaphoreType.DMA((6,))],
        compiler_params=pltpu.CompilerParams(collective_id=0, has_side_effects=True),
        name="gather",
    )(*own)
    full = [o.reshape(8 * o.shape[1], o.shape[2]) for o in out]
    return full[:3], full[3:]


def forward_kernel(x_ref, wg, wu, wd, h1_ref, act_ref, a_ref):
    wide, scale = norm(x_ref[...])
    a = (wide * scale).astype(BF16)
    a_ref[...] = a
    for lo, n in CHUNKS:
        g = dot(a, wg[:, lo : lo + n])
        u = dot(a, wu[:, lo : lo + n])
        act_ref[:, lo : lo + n] = (gated(g)[1] * u).astype(BF16)
    mm = dot(act_ref[...], wd[...]).astype(BF16).astype(F32)
    h1_ref[...] = (wide + mm).astype(BF16)


def forward(x, w):
    return pl.pallas_call(
        forward_kernel,
        grid=(TILES,),
        out_shape=[
            jax.ShapeDtypeStruct((TOK, D), BF16),
            jax.ShapeDtypeStruct((TOK, FF), BF16),
            jax.ShapeDtypeStruct((TOK, D), BF16),
        ],
        in_specs=[rows(D), WHOLE, WHOLE, WHOLE],
        out_specs=[rows(D), rows(FF), rows(D)],
        compiler_params=pltpu.CompilerParams(vmem_limit_bytes=VMEM_LIMIT, dimension_semantics=("arbitrary",)),
        name="forward",
    )(x, *w)


def layer1_kernel(h_ref, dy_ref, act0_ref, wg, wu, wd, dh_ref, og, ou, od, od0, accg, accu, accd, accd0, dgs, dus):
    i = pl.program_id(0)

    @pl.when(i == 0)
    def _():
        for acc in (accg, accu, accd, accd0):
            acc[...] = jnp.zeros_like(acc)

    wide, scale = norm(h_ref[...])
    a = (wide * scale).astype(BF16)
    a_t = a.T
    dy = dy_ref[...]
    dy_t = dy.T
    for lo, n in CHUNKS:
        cut = slice(lo, lo + n)
        g = dot(a, wg[:, cut])
        u = dot(a, wu[:, cut])
        da = dot_nt(dy, wd[cut, :]).astype(BF16).astype(F32)
        sig, si = gated(g)
        act = (si * u).astype(BF16)
        du = (da * si).astype(BF16)
        dg = (da * u * (sig + si * (1.0 - sig))).astype(BF16)
        dgs[:, cut] = dg
        dus[:, cut] = du
        accd[:, cut] += dot(dy_t, act)
        accg[:, cut] += dot(a_t, dg)
        accu[:, cut] += dot(a_t, du)
    dn = (dot_nt(dgs[...], wg[...]) + dot_nt(dus[...], wu[...])).astype(BF16).astype(F32)
    inner = jnp.sum(dn * wide, -1, keepdims=True) * (scale * scale * scale * (1.0 / D))
    by_norm = (dn * scale - wide * inner).astype(BF16).astype(F32)
    dh = (dy.astype(F32) + by_norm).astype(BF16)
    dh_ref[...] = dh
    accd0[...] += dot(dh.T, act0_ref[...])

    @pl.when(i == TILES - 1)
    def _():
        og[...] = accg[...].astype(BF16)
        ou[...] = accu[...].astype(BF16)
        for acc, out in ((accd, od), (accd0, od0)):
            for h in range(2):
                t = acc[256 * h : 256 * h + 256, :].T.astype(BF16)
                for s in range(8):
                    out[s, h] = t[208 * s : 208 * s + 208]


def layer1(h1, dy, act0, w):
    up, down = jax.ShapeDtypeStruct((D, FF), BF16), jax.ShapeDtypeStruct((8, 2, 208, 256), BF16)
    return pl.pallas_call(
        layer1_kernel,
        grid=(TILES,),
        out_shape=[jax.ShapeDtypeStruct((TOK, D), BF16), up, up, down, down],
        in_specs=[rows(D), rows(D), rows(FF), WHOLE, WHOLE, WHOLE],
        out_specs=[rows(D), WHOLE, WHOLE, WHOLE, WHOLE],
        scratch_shapes=[pltpu.VMEM((D, FF), F32)] * 4 + [pltpu.VMEM((TILE, FF), BF16)] * 2,
        compiler_params=pltpu.CompilerParams(vmem_limit_bytes=VMEM_LIMIT, dimension_semantics=("arbitrary",)),
        name="layer1",
    )(h1, dy, act0, *w)


BULK = ((32, FF), (32, FF), (208, 256), (208, 256))
PIECES = BULK + tuple((32, n) for _, n in CHUNKS for _ in range(2))
NP = len(PIECES)
NBUF = 9


def schedule():
    plan = []

    def put(piece, steps):
        for stage, step in enumerate(steps):
            plan.append((min(step, LAST), stage, piece))

    put(0, (0, 2, 9, 15, 19, 22, 25, 99))
    put(1, (0, 2, 9, 15, 19, 22, 25, 99))
    put(2, (0, 4, 14, 20, 24, 27, 30, 99))
    put(3, (0, 4, 14, 20, 24, 27, 30, 99))
    put(4, (8, 10, 18, 23, 26, 29, 31, 99))
    put(5, (8, 10, 18, 23, 26, 29, 31, 99))
    put(6, (16, 18, 22, 26, 29, 31, 99, 99))
    put(7, (16, 18, 22, 26, 29, 31, 99, 99))
    put(8, (24, 26, 29, 31, 99, 99, 99, 99))
    put(9, (24, 26, 29, 31, 99, 99, 99, 99))
    put(10, (99,) * 8)
    put(11, (99,) * 8)
    return sorted(plan, key=lambda e: (e[0], e[1], e[2]))


STEPS = len(CHUNKS) * TILES
LAST = STEPS - 1


def backward0_kernel(*refs):
    a_ref, dh_ref, wg, wu, wd = refs[:5]
    bulk = refs[5:9]
    og, ou, od = refs[9:12]
    a_t, accg, accu = refs[12:15]
    chunk_g = refs[15 : 15 + 2 * len(CHUNKS)]
    at = 15 + 2 * len(CHUNKS)
    bufs = [refs[at + NBUF * k : at + NBUF * (k + 1)] for k in range(NP)]
    send, recv = refs[at + NBUF * NP :]
    terms = list(bulk) + list(chunk_g)

    j, i = pl.program_id(0), pl.program_id(1)
    step = j * TILES + i
    p = Place()
    z = p.z
    outer = (z == 0) | (z == 3)
    inward = jnp.where(z == 0, 1, 2)
    outward = jnp.where(z == 1, 0, 3)
    peer = 3 - z
    half, other = jnp.where(z == 1, 0, 1), jnp.where(z == 1, 1, 0)

    @pl.when(step == 0)
    def _():
        barrier = pltpu.get_barrier_semaphore()
        for n in (p.partner, p.nx, p.ny):
            signal(barrier, p.at(n))

        @pl.when(outer)
        def _():
            signal(barrier, p.at(p.s, inward))
            pl.semaphore_wait(barrier, 4)

        @pl.when(jnp.logical_not(outer))
        def _():
            signal(barrier, p.at(p.s, outward))
            signal(barrier, p.at(p.s, peer))
            pl.semaphore_wait(barrier, 5)

    def piece_stage(k, stage):
        g = terms[k]
        r0, s1, r1, s2, r2, zs, zr, zp, fin = bufs[k]
        x_first = k % 2 == 0
        mine, theirs = (p.x, 1 - p.x) if x_first else (p.y, 1 - p.y)
        mine_b, theirs_b = (p.y, 1 - p.y) if x_first else (p.x, 1 - p.x)
        na, nb = (p.nx, p.ny) if x_first else (p.ny, p.nx)

        def chip(first, second):
            return (first, second) if x_first else (second, first)

        def two(first, second):
            u, v = chip(first, second)
            return g[u, v, p.c].astype(F32) + r0[u, v].astype(F32)

        cps = (
            lambda: copy_to(g.at[:, :, 1 - p.c], r0, send.at[k, 0], recv.at[k, 0], p.at(p.partner)),
            lambda: copy_to(s1, r1, send.at[k, 1], recv.at[k, 1], p.at(na)),
            lambda: copy_to(s2, r2, send.at[k, 2], recv.at[k, 2], p.at(nb)),
        )
        if stage == 0:
            cps[0]().start()
        if stage == 1:
            cps[0]().wait_recv()
            for q in range(2):
                s1[q] = two(theirs, q).astype(BF16)
            cps[1]().start()
        if stage == 2:
            cps[1]().wait_recv()
            s2[...] = (two(mine, theirs_b) + r1[theirs_b].astype(F32)).astype(BF16)
            cps[2]().start()
        to_inner = lambda: copy_to(zs, zr, send.at[k, 3], recv.at[k, 3], p.at(p.s, inward))
        from_outer = lambda: copy_to(zs, zr, send.at[k, 3], recv.at[k, 3], p.at(p.s, outward))
        partial = lambda: copy_to(zs.at[other], zp, send.at[k, 3], recv.at[k, 4], p.at(p.s, peer))
        final_peer = lambda h: copy_to(fin.at[h], fin.at[h], send.at[k, 4], recv.at[k, 5], p.at(p.s, peer))
        final_out = lambda h, n: copy_to(fin.at[h], fin.at[h], send.at[k, 5 + n], recv.at[k, 6 + n], p.at(p.s, outward))
        final_in = lambda h, n: copy_to(fin.at[h], fin.at[h], send.at[k, 5 + n], recv.at[k, 6 + n], p.at(p.s, inward))
        xy_sum = lambda: two(mine, mine_b) + r1[mine_b].astype(F32) + r2[...].astype(F32)
        if stage == 3:
            cps[2]().wait_recv()

            @pl.when(outer)
            def _():
                zs[...] = xy_sum().astype(BF16)
                to_inner().start()

        if stage == 4:

            @pl.when(jnp.logical_not(outer))
            def _():
                from_outer().wait_recv()
                u, v = chip(mine, mine_b)
                total = g[u, v, p.c, other].astype(F32) + r0[u, v, other].astype(F32) + r1[mine_b, other].astype(F32)
                total += r2[other].astype(F32) + zr[other].astype(F32)
                zs[other] = total.astype(BF16)
                partial().start()

        if stage == 5:

            @pl.when(jnp.logical_not(outer))
            def _():
                partial().wait_recv()
                u, v = chip(mine, mine_b)
                total = g[u, v, p.c, half].astype(F32) + r0[u, v, half].astype(F32) + r1[mine_b, half].astype(F32)
                total += r2[half].astype(F32) + zr[half].astype(F32) + zp[...].astype(F32)
                fin[half] = total.astype(BF16)
                final_peer(half).start()
                final_out(half, 0).start()

        if stage == 6:

            @pl.when(jnp.logical_not(outer))
            def _():
                final_peer(other).wait_recv()
                final_out(other, 1).start()

        if stage == 7:

            @pl.when(outer)
            def _():
                final_in(0, 0).wait_recv()
                final_in(1, 1).wait_recv()
                to_inner().wait_send()

            @pl.when(jnp.logical_not(outer))
            def _():
                partial().wait_send()
                final_peer(half).wait_send()
                final_out(half, 0).wait_send()
                final_out(other, 1).wait_send()

            for cp in cps:
                cp().wait_send()
            if k in (0, 1):
                out = (og, ou)[k]
                for h in range(2):
                    out[1, 32 * h : 32 * h + 32, :] = fin[h]
            elif k in (2, 3):
                for h in range(2):
                    od[3 - k, :, 256 * h : 256 * h + 256] = fin[h]
            else:
                lo, n = CHUNKS[(k - 4) // 2]
                for h in range(2):
                    (og, ou)[k % 2][0, 32 * h : 32 * h + 32, lo : lo + n] = fin[h]

    tile = pl.ds(pl.multiple_of(i * TILE, TILE), TILE)

    @pl.when(j == 0)
    def _():
        a_t[i] = a_ref[...].T

    def body(n, lo, first):
        a, dh = a_ref[...], dh_ref[...]
        cut = pl.ds(lo, n)
        g = dot(a, wg[:, cut])
        u = dot(a, wu[:, cut])
        da = dot_nt(dh, wd[cut, :]).astype(BF16).astype(F32)
        sig, si = gated(g)
        du = (da * si).astype(BF16)
        dg = (da * u * (sig + si * (1.0 - sig))).astype(BF16)
        at_tile = a_t[i]
        pg, pu = dot(at_tile, dg), dot(at_tile, du)

        @pl.when(i == 0)
        def _():
            accg[:, :n] = pg
            accu[:, :n] = pu

        @pl.when(i > 0)
        def _():
            accg[:, :n] += pg
            accu[:, :n] += pu

    @pl.when(j < 3)
    def _():
        body(512, pl.multiple_of(j * 512, 512), None)

    @pl.when(j == 3)
    def _():
        body(128, 1536, None)

    for k, (lo, n) in enumerate(CHUNKS):

        @pl.when((j == k) & (i == TILES - 1))
        def _(k=k, n=n):
            for acc, out in ((accg, chunk_g[2 * k]), (accu, chunk_g[2 * k + 1])):
                for q in range(16):
                    c_, h_ = (q // 2) % 2, q % 2
                    out[q // 8, (q // 4) % 2, c_, h_] = acc[32 * q : 32 * q + 32, :n].astype(BF16)

    plan = schedule()
    for now in sorted({e[0] for e in plan}):

        @pl.when(step == now)
        def _(now=now):
            for when, stage, k in plan:
                if when == now:
                    piece_stage(k, stage)


def backward0(a0, dh1, w, bulk):
    tile2 = lambda n: pl.BlockSpec((TILE, n), lambda j, i: (i, 0))
    bufs = []
    for hr, hc in PIECES:
        bufs += [
            pltpu.VMEM((2, 2, 2, hr, hc), BF16),
            pltpu.VMEM((2, 2, hr, hc), BF16),
            pltpu.VMEM((2, 2, hr, hc), BF16),
            pltpu.VMEM((2, hr, hc), BF16),
            pltpu.VMEM((2, hr, hc), BF16),
            pltpu.VMEM((2, hr, hc), BF16),
            pltpu.VMEM((2, hr, hc), BF16),
            pltpu.VMEM((hr, hc), BF16),
            pltpu.VMEM((2, hr, hc), BF16),
        ]
    up, down = jax.ShapeDtypeStruct((2, 64, FF), BF16), jax.ShapeDtypeStruct((2, 208, D), BF16)
    bulk = [t.reshape((2, 2, 2, 2) + shape) for t, shape in zip(bulk, BULK, strict=True)]
    return pl.pallas_call(
        backward0_kernel,
        grid=(len(CHUNKS), TILES),
        out_shape=[up, up, down],
        in_specs=[tile2(D), tile2(D)] + [WHOLE] * 7,
        out_specs=[WHOLE] * 3,
        scratch_shapes=[pltpu.VMEM((TILES, D, TILE), BF16)]
        + [pltpu.VMEM((D, 512), F32)] * 2
        + [pltpu.VMEM((2, 2, 2, 2, 32, n), BF16) for _, n in CHUNKS for _ in range(2)]
        + bufs
        + [pltpu.SemaphoreType.DMA((NP, 7)), pltpu.SemaphoreType.DMA((NP, 8))],
        compiler_params=pltpu.CompilerParams(
            collective_id=1, has_side_effects=True, vmem_limit_bytes=VMEM_LIMIT, dimension_semantics=("arbitrary", "arbitrary")
        ),
        name="backward0",
    )(a0, dh1, *w, *bulk)


def adamw(w, m, v, g):
    m = 0.9 * m + 0.1 * g
    v = 0.95 * v + 0.05 * g * g
    step = m * lax.rsqrt(v + 1e-8) + 0.1 * w
    return (w - 0.02 * step).astype(BF16), m, v


def solution(mesh):
    def step(x, dy, *arrays):
        weights, m, v = (arrays[i : i + 3] for i in (0, 3, 6))
        w0, w1 = gather(weights)
        h1, act0, a0 = forward(x[0], w0)
        dh1, *bulk = layer1(h1, dy[0], act0, w1)
        gradients = backward0(a0, dh1, w0, bulk)
        new = [adamw(w.astype(F32), m, v, g.astype(F32)) for w, m, v, g in zip(weights, m, v, gradients, strict=True)]
        return tuple(one[which] for which in range(3) for one in new)

    states, cut = P(("rep", "r", "s"), None, None), P(None, "s", None)
    return jax.shard_map(
        step,
        mesh=mesh,
        in_specs=(states, states) + (cut,) * 9,
        out_specs=(P("rep", "s", None),) * 9,
        check_vma=False,
    )
```

```python
import functools

import jax
import jax.numpy as jnp
from jax import lax
from jax.experimental import pallas as pl
from jax.experimental.pallas import tpu as pltpu
from jax.sharding import PartitionSpec as P

F32, BF16 = jnp.float32, jnp.bfloat16
D, FF, TOK = 512, 1664, 4096
TILE = 1024
TILES = TOK // TILE
CHUNKS = ((0, 512), (512, 512), (1024, 512), (1536, 128))
VMEM_LIMIT = 66_000_000
ANY = pl.BlockSpec(memory_space=pl.ANY)
WHOLE = pl.BlockSpec(memory_space=pltpu.VMEM)


def dot(a, b):
    return jnp.dot(a, b, preferred_element_type=F32)


def dot_nt(a, b):
    return lax.dot_general(a, b, (((1,), (1,)), ((), ())), preferred_element_type=F32)


def norm(h):
    wide = h.astype(F32)
    scale = lax.rsqrt(jnp.mean(wide * wide, -1, keepdims=True) + 1e-6)
    return wide, scale


def gated(g):
    sig = 0.5 + 0.5 * jnp.tanh(0.5 * g)
    return sig, g * sig


def rows(n):
    return pl.BlockSpec((TILE, n), lambda i: (i, 0))


class Place:
    def __init__(self):
        s, z = lax.axis_index("s"), lax.axis_index("r")
        self.s, self.z = s, z
        self.x, self.y, self.c = s // 4, (s // 2) % 2, s % 2
        x, y, c = self.x, self.y, self.c
        self.partner = x * 4 + y * 2 + (1 - c)
        self.nx = (1 - x) * 4 + y * 2 + c
        self.ny = x * 4 + (1 - y) * 2 + c
        self.diag = (1 - x) * 4 + (1 - y) * 2 + c

    def at(self, s, z=None):
        return (0, self.z if z is None else z, s)


def copy_to(src, dst, send, recv, device):
    return pltpu.make_async_remote_copy(
        src_ref=src, dst_ref=dst, send_sem=send, recv_sem=recv, device_id=device, device_id_type=pl.DeviceIdType.MESH
    )


def signal(barrier, device):
    pl.semaphore_signal(barrier, inc=1, device_id=device, device_id_type=pl.DeviceIdType.MESH)


EARLY = 768
GATHERED = ((0, 0, 0, EARLY), (1, 0, 0, EARLY), (0, 0, EARLY, FF - EARLY), (1, 0, EARLY, FF - EARLY), (2, 0, 0, D))
GATHERED += ((0, 1, 0, FF), (1, 1, 0, FF), (2, 1, 0, D))
NG = len(GATHERED)
FORWARD_STEPS = 3 * TILES
OWN, PASS, DIAG, DONE = range(4)
GATHER_PLAN = {
    0: ((OWN, 0, 1), (PASS, 0, 1), (OWN, 2, 3), (DIAG, 0, 1), (DONE, 0, 1)),
    2: ((PASS, 2, 3), (OWN, 4, 5)),
    4: ((DIAG, 2, 3), (DONE, 2, 3)),
    5: ((PASS, 4), (OWN, 6)),
    6: ((PASS, 5), (OWN, 7)),
    8: ((DIAG, 4), (DONE, 4)),
    9: ((PASS, 6),),
    10: ((DIAG, 5),),
    11: ((PASS, 7),),
    12: ((DIAG, 6, 7), (DONE, 5, 6, 7)),
}


def forward_kernel(og, ou, od, x_ref, h1_ref, act_ref, a_ref, *refs):
    keep, later = refs[:3], refs[3:6]
    w0 = refs[6:9]
    acts, norms = refs[9:11]
    send, recv, local = refs[11:14]
    own = (og, ou, od)
    step = pl.program_id(0)
    p = Place()

    def block(i, slot):
        m, layer, lo, n = GATHERED[i]
        return (later if layer else w0)[m].at[slot, :, pl.ds(lo, n)]

    def cp(i, k):
        m, layer, lo, n = GATHERED[i]
        mine = own[m].at[layer, :, pl.ds(lo, n)]
        src, slot, device = (
            (mine, p.s, p.nx),
            (mine, p.s, p.ny),
            (mine, p.s, p.partner),
            (block(i, p.nx), p.nx, p.partner),
            (block(i, p.ny), p.ny, p.partner),
            (block(i, p.nx), p.nx, p.ny) if i % 2 == 0 else (block(i, p.ny), p.ny, p.nx),
            (block(i, p.diag), p.diag, p.partner),
        )[k]
        return copy_to(src, block(i, slot), send.at[i, k], recv.at[i, k], p.at(device))

    def do(what, i):
        if what == OWN:
            for k in range(3):
                cp(i, k).start()
        elif what == PASS:
            first, then = (0, 1) if i % 2 == 0 else (1, 0)
            cp(i, first).wait_recv()
            cp(i, 5).start()
            cp(i, 3 + first).start()
            cp(i, then).wait_recv()
            cp(i, 3 + then).start()
        elif what == DIAG:
            cp(i, 5).wait_recv()
            cp(i, 6).start()
        else:
            for k in (2, 3, 4, 6):
                cp(i, k).wait_recv()

    def follow(now):
        for what, *items in GATHER_PLAN[now]:
            for i in items:
                do(what, i)

    def own_out(m):
        return pltpu.make_async_copy(own[m].at[1], later[m].at[p.s], local.at[m])

    def w0_out(m):
        return pltpu.make_async_copy(w0[m], keep[m], local.at[3 + m])

    def act_out(t):
        return pltpu.make_async_copy(acts.at[t], act_ref.at[pl.ds(t * TILE, TILE)], local.at[6 + t])

    def norm_out(t):
        return pltpu.make_async_copy(norms.at[t], a_ref.at[pl.ds(t * TILE, TILE)], local.at[6 + TILES + t])

    @pl.when(step == 0)
    def _():
        barrier = pltpu.get_barrier_semaphore()
        for n in (p.partner, p.nx, p.ny):
            signal(barrier, p.at(n))
        pl.semaphore_wait(barrier, 3)
        for m in range(3):
            w0[m][p.s] = own[m][0]
            own_out(m).start()

    @pl.when(step < TILES)
    def _():
        wide, scale = norm(x_ref[...])
        norms[step] = (wide * scale).astype(BF16)

    for now in GATHER_PLAN:
        if now < FORWARD_STEPS:
            pl.when(step == now)(functools.partial(follow, now))

    def up(t, lo, n):
        g = dot(norms[t], w0[0][:, :, lo : lo + n].reshape(D, n))
        u = dot(norms[t], w0[1][:, :, lo : lo + n].reshape(D, n))
        acts[t, :, lo : lo + n] = (gated(g)[1] * u).astype(BF16)

    @pl.when(step < TILES)
    def _():
        up(step, 0, EARLY)

    @pl.when((step >= TILES) & (step < 2 * TILES))
    def _():
        up(step - TILES, EARLY, FF - EARLY)

    @pl.when(step >= 2 * TILES)
    def _():
        mm = dot(acts[step - 2 * TILES], w0[2][...].reshape(FF, D)).astype(BF16).astype(F32)
        h1_ref[...] = (x_ref[...].astype(F32) + mm).astype(BF16)

    for k in range(TILES):

        @pl.when(step == TILES + 1 + k)
        def _(k=k):
            act_out(k).start()
            norm_out(k).start()

    @pl.when(step == 2 * TILES + 1)
    def _():
        for m in range(3):
            w0_out(m).start()

    @pl.when(step == FORWARD_STEPS - 1)
    def _():
        follow(FORWARD_STEPS)
        for i in range(NG):
            for k in range(7):
                cp(i, k).wait_send()
        for m in range(3):
            own_out(m).wait()
            w0_out(m).wait()
        for k in range(TILES):
            act_out(k).wait()
            norm_out(k).wait()


def forward(x, weights):
    blocks = [jax.ShapeDtypeStruct((8,) + w.shape[1:], BF16) for w in weights]
    h1, act, a, *full = pl.pallas_call(
        forward_kernel,
        grid=(FORWARD_STEPS,),
        out_shape=[
            jax.ShapeDtypeStruct((TOK, D), BF16),
            jax.ShapeDtypeStruct((TOK, FF), BF16),
            jax.ShapeDtypeStruct((TOK, D), BF16),
        ]
        + blocks * 2,
        in_specs=[WHOLE, WHOLE, WHOLE, pl.BlockSpec((TILE, D), lambda n: (jnp.where(n < TILES, n, jnp.maximum(n - 2 * TILES, 0)), 0))],
        out_specs=[pl.BlockSpec((TILE, D), lambda n: (jnp.maximum(n - 2 * TILES, 0), 0))] + [ANY] * 8,
        scratch_shapes=[pltpu.VMEM(b.shape, BF16) for b in blocks]
        + [pltpu.VMEM((TILES, TILE, FF), BF16), pltpu.VMEM((TILES, TILE, D), BF16)]
        + [pltpu.SemaphoreType.DMA((NG, 7)), pltpu.SemaphoreType.DMA((NG, 7)), pltpu.SemaphoreType.DMA((6 + 2 * TILES,))],
        compiler_params=pltpu.CompilerParams(
            collective_id=0, has_side_effects=True, vmem_limit_bytes=VMEM_LIMIT, dimension_semantics=("arbitrary",)
        ),
        name="forward",
    )(*weights, x)
    full = [o.reshape(8 * o.shape[1], o.shape[2]) for o in full]
    return h1, act, a, full[:3], full[3:]


def layer1_kernel(h_ref, dy_ref, act0_ref, wg, wu, wd, dh_ref, og, ou, od, od0, accg, accu, accd, accd0, dgs, dus):
    i = pl.program_id(0)

    @pl.when(i == 0)
    def _():
        for acc in (accg, accu, accd, accd0):
            acc[...] = jnp.zeros_like(acc)

    wide, scale = norm(h_ref[...])
    a = (wide * scale).astype(BF16)
    a_t = a.T
    dy = dy_ref[...]
    dy_t = dy.T
    for lo, n in CHUNKS:
        cut = slice(lo, lo + n)
        g = dot(a, wg[:, cut])
        u = dot(a, wu[:, cut])
        da = dot_nt(dy, wd[cut, :]).astype(BF16).astype(F32)
        sig, si = gated(g)
        act = (si * u).astype(BF16)
        du = (da * si).astype(BF16)
        dg = (da * u * (sig + si * (1.0 - sig))).astype(BF16)
        dgs[:, cut] = dg
        dus[:, cut] = du
        accd[:, cut] += dot(dy_t, act)
        accg[:, cut] += dot(a_t, dg)
        accu[:, cut] += dot(a_t, du)
    dn = (dot_nt(dgs[...], wg[...]) + dot_nt(dus[...], wu[...])).astype(BF16).astype(F32)
    inner = jnp.sum(dn * wide, -1, keepdims=True) * (scale * scale * scale * (1.0 / D))
    by_norm = (dn * scale - wide * inner).astype(BF16).astype(F32)
    dh = (dy.astype(F32) + by_norm).astype(BF16)
    dh_ref[...] = dh
    accd0[...] += dot(dh.T, act0_ref[...])

    @pl.when(i == TILES - 1)
    def _():
        og[...] = accg[...].astype(BF16)
        ou[...] = accu[...].astype(BF16)
        for acc, out in ((accd, od), (accd0, od0)):
            for h in range(4):
                t = acc[128 * h : 128 * h + 128, :].T.astype(BF16)
                for s in range(8):
                    out[s, h] = t[208 * s : 208 * s + 208]


def layer1(h1, dy, act0, w):
    up, down = jax.ShapeDtypeStruct((D, FF), BF16), jax.ShapeDtypeStruct((8, 4, 208, 128), BF16)
    return pl.pallas_call(
        layer1_kernel,
        grid=(TILES,),
        out_shape=[jax.ShapeDtypeStruct((TOK, D), BF16), up, up, down, down],
        in_specs=[rows(D), rows(D), rows(FF), WHOLE, WHOLE, WHOLE],
        out_specs=[rows(D), WHOLE, WHOLE, WHOLE, WHOLE],
        scratch_shapes=[pltpu.VMEM((D, FF), F32)] * 4 + [pltpu.VMEM((TILE, FF), BF16)] * 2,
        compiler_params=pltpu.CompilerParams(vmem_limit_bytes=VMEM_LIMIT, dimension_semantics=("arbitrary",)),
        name="layer1",
    )(h1, dy, act0, *w)


BULK = ((16, FF),) * 4 + ((208, 128),) * 4
PIECES = BULK + tuple((32, n) for _, n in CHUNKS for _ in range(2))
NP = len(PIECES)
NBUF = 10
DIRECT = NP - 2


def schedule():
    plan = []

    def put(pieces, *steps):
        for piece in pieces:
            for stage, step in enumerate(steps + (99,) * (LAST + 1 - len(steps))):
                plan.append((min(step, STEPS), stage, piece))

    put((0, 1), 0, 0, 2, 4, 6, 8)
    put((2, 3), 0, 1, 3, 6, 8, 10)
    put((4, 5), 0, 2, 5, 8, 10, 12)
    put((6, 7), 0, 3, 7, 9, 11, 13)
    put((8, 9), 4, 5, 8, 10, 12, 14)
    put((10, 11), 8, 9, 11, 13, 15)
    put((12, 13), 12, 13, 15)
    put((14, 15), 16)
    def rank(e):
        step, stage, piece = e
        if step == STEPS:
            return (step, (0, 1, 3.5, 5.5, 9, 9, 9)[stage] if piece >= DIRECT else max(stage, 2.5), piece)
        return (step, stage, piece) if step == 0 else (step, piece // 2, stage, piece)

    return sorted(plan, key=rank)


LAST = 6
STEPS = len(CHUNKS) * TILES


def backward0_kernel(*refs):
    a_ref, dh_ref = refs[:2]
    hbm_w = refs[2:5]
    bulk = refs[5:9]
    og, ou, od = refs[9:12]
    a_t, accg, accu = refs[12:15]
    chunk_g = refs[15 : 15 + 2 * len(CHUNKS)]
    at = 15 + 2 * len(CHUNKS)
    bulk_own = refs[at : at + 8]
    at += 8
    bufs = [refs[at + NBUF * k : at + NBUF * (k + 1)] for k in range(NP)]
    wg, wu, wd, send, recv, local = refs[at + NBUF * NP :]
    loads = lambda: [pltpu.make_async_copy(a, b, local.at[8 + n]) for n, (a, b) in enumerate(zip(hbm_w, (wg, wu, wd), strict=True))]

    j, i = pl.program_id(0), pl.program_id(1)
    step = j * TILES + i
    p = Place()
    z = p.z
    beside, across = z + 1 - 2 * (z % 2), 3 - z
    half_beside, half_across = (z + z // 2) % 2, z // 2

    @pl.when(step == 0)
    def _():
        barrier = pltpu.get_barrier_semaphore()
        for n in (p.partner, p.nx, p.ny, p.diag):
            signal(barrier, p.at(n))
        for n in range(1, 4):
            signal(barrier, p.at(p.s, lax.rem(z + n, 4)))
        pl.semaphore_wait(barrier, 7)
        for cp in loads():
            cp.start()

    def piece_stage(k, stage):
        r0, s1, r1, s2, r2, zs, zr, zt, zp, fin = bufs[k]
        one, two_, half = (beside, across, half_beside) if (k // 2) % 2 == 0 else (across, beside, half_across)
        other = 1 - half
        x_first = k % 2 == 0
        mine, theirs = (p.x, 1 - p.x) if x_first else (p.y, 1 - p.y)
        mine_b, theirs_b = (p.y, 1 - p.y) if x_first else (p.x, 1 - p.x)
        na, nb = (p.nx, p.ny) if x_first else (p.ny, p.nx)

        def chip(first, second):
            return (first, second) if x_first else (second, first)

        if k < 8:
            source = bulk[k // 2].at[:, :, 1 - p.c, k % 2]
            own_half = lambda: pltpu.make_async_copy(bulk[k // 2].at[:, :, p.c, k % 2], bulk_own[k], local.at[k])
            term = lambda u, v: bulk_own[k][u, v].astype(F32)
            term_half = lambda u, v, h: bulk_own[k][u, v, h].astype(F32)
        else:
            source = chunk_g[k - 8].at[:, :, 1 - p.c]
            own_half = None
            term = lambda u, v: chunk_g[k - 8][u, v, p.c].astype(F32)
            term_half = lambda u, v, h: chunk_g[k - 8][u, v, p.c, h].astype(F32)

        def two(first, second):
            u, v = chip(first, second)
            return term(u, v) + r0[u, v].astype(F32)

        cps = (
            lambda: copy_to(source, r0, send.at[k, 0], recv.at[k, 0], p.at(p.partner)),
            lambda: copy_to(s1, r1, send.at[k, 1], recv.at[k, 1], p.at(na)),
            lambda: copy_to(s2, r2, send.at[k, 2], recv.at[k, 2], p.at(nb)),
        )
        def finish():
            for h in range(2):
                if k < 4:
                    lo = 32 * (k % 2) + 16 * h
                    (og, ou)[k // 2][1, lo : lo + 16, :] = fin[h]
                elif k < 8:
                    lo = 256 * (k % 2) + 128 * h
                    od[(7 - k) // 2, :, lo : lo + 128] = fin[h]
                else:
                    lo, n = CHUNKS[(k - 8) // 2]
                    (og, ou)[k % 2][0, 32 * h : 32 * h + 32, lo : lo + n] = fin[h]

        if k >= DIRECT:
            chips = ((1 - p.x, p.y), (p.x, 1 - p.y), (1 - p.x, 1 - p.y))
            across_chips = [
                lambda n=n, u=u, v=v: copy_to(
                    s1.at[n], r1.at[n], send.at[k, 1 + n], recv.at[k, 1 + n], p.at(u * 4 + v * 2 + p.c)
                )
                for n, (u, v) in enumerate(chips)
            ]
            along = [
                lambda n=n: copy_to(zs.at[z], zs.at[z], send.at[k, 4 + n], recv.at[k, 4 + n], p.at(p.s, lax.rem(z + 1 + n, 4)))
                for n in range(3)
            ]
            arrived = [
                lambda n=n: copy_to(zs.at[lax.rem(z + 3 - n, 4)], zs.at[lax.rem(z + 3 - n, 4)], send.at[k, 4 + n], recv.at[k, 4 + n], p.at(p.s, lax.rem(z + 3 - n, 4)))
                for n in range(3)
            ]
            if stage == 0:
                cps[0]().start()
            if stage == 1:
                cps[0]().wait_recv()
                for n in (2, 0, 1):
                    s1[n] = two(*chip(*chips[n])).astype(BF16)
                    across_chips[n]().start()
            if stage == 2:
                for cp in across_chips:
                    cp().wait_recv()
                total = two(*chip(p.x, p.y))
                for n in range(3):
                    total += r1[n].astype(F32)
                zs[z] = total.astype(BF16)
                for cp in along:
                    cp().start()
            if stage == 3:
                for cp in arrived:
                    cp().wait_recv()
                total = zs[0].astype(F32) + zs[1].astype(F32) + zs[2].astype(F32) + zs[3].astype(F32)
                fin[...] = total.astype(BF16)
                finish()
            if stage == 4:
                for cp in [cps[0]] + across_chips + along:
                    cp().wait_send()
            return

        if stage == 0:
            cps[0]().start()
            if own_half is not None:
                own_half().start()
        if stage == 1:
            cps[0]().wait_recv()
            if own_half is not None:
                own_half().wait()
            for q in range(2):
                s1[q] = two(theirs, q).astype(BF16)
            cps[1]().start()
        if stage == 2:
            cps[1]().wait_recv()
            s2[...] = (two(mine, theirs_b) + r1[theirs_b].astype(F32)).astype(BF16)
            cps[2]().start()
        z_cps = (
            lambda: copy_to(zs, zr, send.at[k, 3], recv.at[k, 3], p.at(p.s, one)),
            lambda: copy_to(zt, zp, send.at[k, 4], recv.at[k, 4], p.at(p.s, two_)),
            lambda: copy_to(fin.at[half], fin.at[half], send.at[k, 5], recv.at[k, 5], p.at(p.s, one)),
        )

        def xy_sum(h):
            u, v = chip(mine, mine_b)
            return term_half(u, v, h) + r0[u, v, h].astype(F32) + r1[mine_b, h].astype(F32) + r2[h].astype(F32)

        if stage == 3:
            cps[2]().wait_recv()
            zs[...] = xy_sum(other).astype(BF16)
            z_cps[0]().start()
        if stage == 4:
            z_cps[0]().wait_recv()
            zt[...] = (xy_sum(half) + zr[...].astype(F32)).astype(BF16)
            z_cps[1]().start()
        if stage == 5:
            z_cps[1]().wait_recv()
            fin[half] = (zt[...].astype(F32) + zp[...].astype(F32)).astype(BF16)
            z_cps[2]().start()
        if stage == 6:
            copy_to(fin.at[other], fin.at[other], send.at[k, 5], recv.at[k, 5], p.at(p.s, one)).wait_recv()
            for cp in z_cps:
                cp().wait_send()
            for cp in cps:
                cp().wait_send()
            finish()

    plan = schedule()

    def events(now):
        for when, stage, k in plan:
            if when == now:
                piece_stage(k, stage)

    for now in sorted({e[0] for e in plan if e[0] < STEPS}):
        pl.when(step == now)(functools.partial(events, now))

    @pl.when(step == 0)
    def _():
        for cp in loads():
            cp.wait()

    @pl.when(j == 0)
    def _():
        a_t[i] = a_ref[...].T

    def body(n, lo, first):
        a, dh = a_ref[...], dh_ref[...]
        cut = pl.ds(lo, n)
        g = dot(a, wg[:, cut])
        u = dot(a, wu[:, cut])
        da = dot_nt(dh, wd[cut, :]).astype(BF16).astype(F32)
        sig, si = gated(g)
        du = (da * si).astype(BF16)
        dg = (da * u * (sig + si * (1.0 - sig))).astype(BF16)
        at_tile = a_t[i]
        pg, pu = dot(at_tile, dg), dot(at_tile, du)

        @pl.when(i == 0)
        def _():
            accg[:, :n] = pg
            accu[:, :n] = pu

        @pl.when(i > 0)
        def _():
            accg[:, :n] += pg
            accu[:, :n] += pu

    @pl.when(j < 3)
    def _():
        body(512, pl.multiple_of(j * 512, 512), None)

    @pl.when(j == 3)
    def _():
        body(128, 1536, None)

    for k, (lo, n) in enumerate(CHUNKS):

        @pl.when((j == k) & (i == TILES - 1))
        def _(k=k, n=n):
            for acc, out in ((accg, chunk_g[2 * k]), (accu, chunk_g[2 * k + 1])):
                for q in range(16):
                    c_, h_ = (q // 2) % 2, q % 2
                    out[q // 8, (q // 4) % 2, c_, h_] = acc[32 * q : 32 * q + 32, :n].astype(BF16)

    pl.when(step == STEPS - 1)(functools.partial(events, STEPS))


def backward0(a0, dh1, w, bulk):
    tile2 = lambda n: pl.BlockSpec((TILE, n), lambda j, i: (i, 0))
    bufs = []
    for k, (hr, hc) in enumerate(PIECES):
        one, four = (hr, hc), (2, 2, hr, hc)
        if k < DIRECT:
            shapes = (2,) + four, four, four, (2,) + one, (2,) + one, one, one, one, one, (2,) + one
        else:
            shapes = (2,) + four, (3, 2) + one, (3, 2) + one, one, one, (4, 2) + one, one, one, one, (2,) + one
        bufs += [pltpu.VMEM(shape, BF16) for shape in shapes]
    up, down = jax.ShapeDtypeStruct((2, 64, FF), BF16), jax.ShapeDtypeStruct((2, 208, D), BF16)
    bulk = [t.reshape((2, 2, 2, 2, 2) + shape) for t, shape in zip(bulk, BULK[::2], strict=True)]
    return pl.pallas_call(
        backward0_kernel,
        grid=(len(CHUNKS), TILES),
        out_shape=[up, up, down],
        in_specs=[tile2(D), tile2(D)] + [ANY] * 7,
        out_specs=[WHOLE] * 3,
        scratch_shapes=[pltpu.VMEM((TILES, D, TILE), BF16)]
        + [pltpu.VMEM((D, 512), F32)] * 2
        + [pltpu.VMEM((2, 2, 2, 2, 32, n), BF16) for _, n in CHUNKS for _ in range(2)]
        + [pltpu.VMEM((2, 2, 2) + shape, BF16) for shape in BULK]
        + bufs
        + [pltpu.VMEM((D, FF), BF16), pltpu.VMEM((D, FF), BF16), pltpu.VMEM((FF, D), BF16)]
        + [pltpu.SemaphoreType.DMA((NP, 7)), pltpu.SemaphoreType.DMA((NP, 7)), pltpu.SemaphoreType.DMA((11,))],
        compiler_params=pltpu.CompilerParams(
            collective_id=1, has_side_effects=True, vmem_limit_bytes=VMEM_LIMIT, dimension_semantics=("arbitrary", "arbitrary")
        ),
        name="backward0",
    )(a0, dh1, *w, *bulk)


def adamw(w, m, v, g):
    m = 0.9 * m + 0.1 * g
    v = 0.95 * v + 0.05 * g * g
    step = m * lax.rsqrt(v + 1e-8) + 0.1 * w
    return (w - 0.02 * step).astype(BF16), m, v


def solution(mesh):
    def step(x, dy, *arrays):
        weights, m, v = (arrays[i : i + 3] for i in (0, 3, 6))
        h1, act0, a0, w0, w1 = forward(x[0], weights)
        dh1, *bulk = layer1(h1, dy[0], act0, w1)
        gradients = backward0(a0, dh1, w0, bulk)
        new = [adamw(w.astype(F32), m, v, g.astype(F32)) for w, m, v, g in zip(weights, m, v, gradients, strict=True)]
        return tuple(one[which] for which in range(3) for one in new)

    states, cut = P(("rep", "r", "s"), None, None), P(None, "s", None)
    return jax.shard_map(
        step,
        mesh=mesh,
        in_specs=(states, states) + (cut,) * 9,
        out_specs=(P("rep", "s", None),) * 9,
        check_vma=False,
    )
```

```python
import functools

import jax
import jax.numpy as jnp
from jax import lax
from jax.experimental import pallas as pl
from jax.experimental.pallas import tpu as pltpu
from jax.sharding import PartitionSpec as P

F32, BF16 = jnp.float32, jnp.bfloat16
D, FF, TOK = 512, 1664, 4096
TILE = 1024
STRIP = 256
TILES = TOK // TILE
CHUNKS = ((0, 512), (512, 512), (1024, 512), (1536, 128))
VMEM_LIMIT = 66_000_000
ANY = pl.BlockSpec(memory_space=pl.ANY)
WHOLE = pl.BlockSpec(memory_space=pltpu.VMEM)


def pieces_of(lo, n):
    return [(lo + at, min(STRIP, n - at)) for at in range(0, n, STRIP)]


def dot(a, b):
    return jnp.dot(a, b, preferred_element_type=F32)


def dot_nt(a, b):
    return lax.dot_general(a, b, (((1,), (1,)), ((), ())), preferred_element_type=F32)


def norm(h):
    wide = h.astype(F32)
    scale = lax.rsqrt(jnp.mean(wide * wide, -1, keepdims=True) + 1e-6)
    return wide, scale


def gated(g):
    sig = 0.5 + 0.5 * jnp.tanh(0.5 * g)
    return sig, g * sig


def rows(n):
    return pl.BlockSpec((TILE, n), lambda i: (i, 0))


class Place:
    def __init__(self):
        s, z = lax.axis_index("s"), lax.axis_index("r")
        self.s, self.z = s, z
        self.x, self.y, self.c = s // 4, (s // 2) % 2, s % 2
        x, y, c = self.x, self.y, self.c
        self.x_, self.y_, self.c_ = 1 - x, 1 - y, 1 - c
        self.partner = self.core(x, y, self.c_)
        self.nx = self.core(self.x_, y, c)
        self.ny = self.core(x, self.y_, c)
        self.diag = self.core(self.x_, self.y_, c)

    @staticmethod
    def core(x, y, c):
        return x * 4 + y * 2 + c

    def at(self, s, z=None):
        return (0, self.z if z is None else z, s)


def copy_to(src, dst, send, recv, device):
    return pltpu.make_async_remote_copy(
        src_ref=src, dst_ref=dst, send_sem=send, recv_sem=recv, device_id=device, device_id_type=pl.DeviceIdType.MESH
    )


def signal(barrier, device):
    pl.semaphore_signal(barrier, inc=1, device_id=device, device_id_type=pl.DeviceIdType.MESH)


EARLY = 768
GATHERED = tuple((m, 0, lo, n) for lo, n in ((0, EARLY), (EARLY, FF - EARLY)) for m in (0, 1)) + ((2, 0, 0, D),)
GATHERED += tuple((m, 1, 0, n) for m, n in enumerate((FF, FF, D)))
NG = len(GATHERED)
FORWARD_STEPS = 3 * TILES
OWN, PASS, DIAG, DONE = range(4)
GATHER_PLAN = {
    0: ((OWN, 0, 1), (PASS, 0, 1), (OWN, 2, 3), (DIAG, 0, 1), (DONE, 0, 1)),
    2: ((PASS, 2, 3), (OWN, 4, 5)),
    4: ((DIAG, 2, 3), (DONE, 2, 3)),
    5: ((PASS, 4), (OWN, 6)),
    6: ((PASS, 5), (OWN, 7)),
    8: ((DIAG, 4), (DONE, 4)),
    9: ((PASS, 6),),
    10: ((DIAG, 5),),
    11: ((PASS, 7),),
    12: ((DIAG, 6, 7), (DONE, 5, 6, 7)),
}


def forward_kernel(og, ou, od, x_ref, h1_ref, act_ref, a_ref, *refs):
    keep, later = refs[:3], refs[3:6]
    w0 = refs[6:9]
    acts, norms = refs[9:11]
    send, recv, local = refs[11:14]
    own = (og, ou, od)
    step = pl.program_id(0)
    p = Place()

    def block(i, slot):
        m, layer, lo, n = GATHERED[i]
        return (later if layer else w0)[m].at[slot, :, pl.ds(lo, n)]

    def cp(i, k):
        m, layer, lo, n = GATHERED[i]
        mine = own[m].at[layer, :, pl.ds(lo, n)]
        src, slot, device = (
            (mine, p.s, p.nx),
            (mine, p.s, p.ny),
            (mine, p.s, p.partner),
            (block(i, p.nx), p.nx, p.partner),
            (block(i, p.ny), p.ny, p.partner),
            (block(i, p.nx), p.nx, p.ny) if i % 2 == 0 else (block(i, p.ny), p.ny, p.nx),
            (block(i, p.diag), p.diag, p.partner),
        )[k]
        return copy_to(src, block(i, slot), send.at[i, k], recv.at[i, k], p.at(device))

    def do(what, i):
        if what == OWN:
            for k in range(3):
                cp(i, k).start()
        elif what == PASS:
            first, then = (0, 1) if i % 2 == 0 else (1, 0)
            cp(i, first).wait_recv()
            cp(i, 5).start()
            cp(i, 3 + first).start()
            cp(i, then).wait_recv()
            cp(i, 3 + then).start()
        elif what == DIAG:
            cp(i, 5).wait_recv()
            cp(i, 6).start()
        else:
            for k in (2, 3, 4, 6):
                cp(i, k).wait_recv()

    def follow(now):
        for what, *items in GATHER_PLAN[now]:
            for i in items:
                do(what, i)

    def own_out(m):
        return pltpu.make_async_copy(own[m].at[1], later[m].at[p.s], local.at[m])

    def w0_out(m):
        return pltpu.make_async_copy(w0[m], keep[m], local.at[3 + m])

    def act_out(t):
        return pltpu.make_async_copy(acts.at[t], act_ref.at[pl.ds(t * TILE, TILE)], local.at[6 + t])

    def norm_out(t):
        return pltpu.make_async_copy(norms.at[t], a_ref.at[pl.ds(t * TILE, TILE)], local.at[6 + TILES + t])

    @pl.when(step == 0)
    def _():
        barrier = pltpu.get_barrier_semaphore()
        for n in (p.partner, p.nx, p.ny):
            signal(barrier, p.at(n))
        pl.semaphore_wait(barrier, 3)
        for m in range(3):
            w0[m][p.s] = own[m][0]
            own_out(m).start()

    @pl.when(step < TILES)
    def _():
        wide, scale = norm(x_ref[...])
        norms[step] = (wide * scale).astype(BF16)

    for now in GATHER_PLAN:
        if now < FORWARD_STEPS:
            pl.when(step == now)(functools.partial(follow, now))

    def up(t, lo, n):
        for at, width in pieces_of(lo, n):
            cut = slice(at, at + width)
            g = dot(norms[t], w0[0][:, :, cut].reshape(D, width))
            u = dot(norms[t], w0[1][:, :, cut].reshape(D, width))
            acts[t, :, cut] = (gated(g)[1] * u).astype(BF16)

    @pl.when(step < TILES)
    def _():
        up(step, 0, EARLY)

    @pl.when((step >= TILES) & (step < 2 * TILES))
    def _():
        up(step - TILES, EARLY, FF - EARLY)

    @pl.when(step >= 2 * TILES)
    def _():
        mm = dot(acts[step - 2 * TILES], w0[2][...].reshape(FF, D)).astype(BF16).astype(F32)
        h1_ref[...] = (x_ref[...].astype(F32) + mm).astype(BF16)

    for k in range(TILES):

        @pl.when(step == TILES + 1 + k)
        def _(k=k):
            act_out(k).start()
            norm_out(k).start()

    @pl.when(step == 2 * TILES + 1)
    def _():
        for m in range(3):
            w0_out(m).start()

    @pl.when(step == FORWARD_STEPS - 1)
    def _():
        follow(FORWARD_STEPS)
        for i in range(NG):
            for k in range(7):
                cp(i, k).wait_send()
        for m in range(3):
            own_out(m).wait()
            w0_out(m).wait()
        for k in range(TILES):
            act_out(k).wait()
            norm_out(k).wait()


def forward(x, weights):
    blocks = [jax.ShapeDtypeStruct((8,) + w.shape[1:], BF16) for w in weights]
    h1, act, a, *full = pl.pallas_call(
        forward_kernel,
        grid=(FORWARD_STEPS,),
        out_shape=[
            jax.ShapeDtypeStruct((TOK, D), BF16),
            jax.ShapeDtypeStruct((TOK, FF), BF16),
            jax.ShapeDtypeStruct((TOK, D), BF16),
        ]
        + blocks * 2,
        in_specs=[WHOLE, WHOLE, WHOLE, pl.BlockSpec((TILE, D), lambda n: (jnp.where(n < TILES, n, jnp.maximum(n - 2 * TILES, 0)), 0))],
        out_specs=[pl.BlockSpec((TILE, D), lambda n: (jnp.maximum(n - 2 * TILES, 0), 0))] + [ANY] * 8,
        scratch_shapes=[pltpu.VMEM(b.shape, BF16) for b in blocks]
        + [pltpu.VMEM((TILES, TILE, FF), BF16), pltpu.VMEM((TILES, TILE, D), BF16)]
        + [pltpu.SemaphoreType.DMA((NG, 7)), pltpu.SemaphoreType.DMA((NG, 7)), pltpu.SemaphoreType.DMA((6 + 2 * TILES,))],
        compiler_params=pltpu.CompilerParams(
            collective_id=0, has_side_effects=True, vmem_limit_bytes=VMEM_LIMIT, dimension_semantics=("arbitrary",)
        ),
        name="forward",
    )(*weights, x)
    full = [o.reshape(8 * o.shape[1], o.shape[2]) for o in full]
    return h1, act, a, full[:3], full[3:]


def layer1_kernel(h_ref, dy_ref, act0_ref, wg, wu, wd, dh_ref, og, ou, od, od0, accg, accu, accd, accd0, dgs, dus, acts):
    i = pl.program_id(0)

    @pl.when(i == 0)
    def _():
        for acc in (accg, accu, accd, accd0):
            acc[...] = jnp.zeros_like(acc)

    wide, scale = norm(h_ref[...])
    a = (wide * scale).astype(BF16)
    a_t = a.T
    dy = dy_ref[...]
    dy_t = dy.T
    for lo, n in pieces_of(0, FF):
        cut = slice(lo, lo + n)
        g = dot(a, wg[:, cut])
        u = dot(a, wu[:, cut])
        da = dot_nt(dy, wd[cut, :]).astype(BF16).astype(F32)
        sig, si = gated(g)
        act = (si * u).astype(BF16)
        du = (da * si).astype(BF16)
        dg = (da * u * (sig + si * (1.0 - sig))).astype(BF16)
        dgs[:, cut] = dg
        dus[:, cut] = du
        acts[:, cut] = act
    accd[...] += dot(dy_t, acts[...])
    accg[...] += dot(a_t, dgs[...])
    accu[...] += dot(a_t, dus[...])
    dn = (dot_nt(dgs[...], wg[...]) + dot_nt(dus[...], wu[...])).astype(BF16).astype(F32)
    inner = jnp.sum(dn * wide, -1, keepdims=True) * (scale * scale * scale * (1.0 / D))
    by_norm = (dn * scale - wide * inner).astype(BF16).astype(F32)
    dh = (dy.astype(F32) + by_norm).astype(BF16)
    dh_ref[...] = dh
    accd0[...] += dot(dh.T, act0_ref[...])

    @pl.when(i == TILES - 1)
    def _():
        og[...] = accg[...].astype(BF16)
        ou[...] = accu[...].astype(BF16)
        for acc, out in ((accd, od), (accd0, od0)):
            for h in range(4):
                t = acc[128 * h : 128 * h + 128, :].T.astype(BF16)
                for s in range(8):
                    out[s, h] = t[208 * s : 208 * s + 208]


def layer1(h1, dy, act0, w):
    up, down = jax.ShapeDtypeStruct((D, FF), BF16), jax.ShapeDtypeStruct((8, 4, 208, 128), BF16)
    return pl.pallas_call(
        layer1_kernel,
        grid=(TILES,),
        out_shape=[jax.ShapeDtypeStruct((TOK, D), BF16), up, up, down, down],
        in_specs=[rows(D), rows(D), rows(FF), WHOLE, WHOLE, WHOLE],
        out_specs=[rows(D), WHOLE, WHOLE, WHOLE, WHOLE],
        scratch_shapes=[pltpu.VMEM((D, FF), F32)] * 4 + [pltpu.VMEM((TILE, FF), BF16)] * 3,
        compiler_params=pltpu.CompilerParams(vmem_limit_bytes=VMEM_LIMIT, dimension_semantics=("arbitrary",)),
        name="layer1",
    )(h1, dy, act0, *w)


BULK = ((16, FF),) * 4 + ((208, 128),) * 4
PIECES = BULK + tuple((32, n) for _, n in CHUNKS for _ in range(2))
NP = len(PIECES)
NBUF = 10
DIRECT = NP - 2


def schedule():
    plan = []

    def put(pair, *steps):
        for piece in (pair, pair + 1):
            for stage in range(STAGES):
                plan.append((steps[stage] if stage < len(steps) else STEPS, stage, piece))

    put(0, 0, 0, 2, 4, 6, 8)
    put(2, 0, 1, 3, 6, 8, 10)
    put(4, 0, 2, 5, 8, 11, 13)
    put(6, 0, 3, 7, 9, 12, 14)
    put(8, 4, 5, 8, 10, 13, 15)
    put(10, 8, 9, 11, 13, 15)
    put(12, 12, 13, 15)
    put(14)
    def rank(e):
        step, stage, piece = e
        if step == STEPS:
            return (step, (stage if stage < 2 else 4 * stage - 1) if piece >= DIRECT else 2 * stage, piece)
        return (step, stage, piece) if step == 0 else (step, piece // 2, stage, piece)

    return sorted(plan, key=rank)


STAGES = 7
STEPS = len(CHUNKS) * TILES


def backward0_kernel(*refs):
    a_ref, dh_ref = refs[:2]
    hbm_w = refs[2:5]
    bulk = refs[5:9]
    og, ou, od = refs[9:12]
    a_t, accg, accu = refs[12:15]
    chunk_g = refs[15 : 15 + 2 * len(CHUNKS)]
    at = 15 + 2 * len(CHUNKS)
    bulk_own = refs[at : at + 8]
    at += 8
    bufs = [refs[at + NBUF * k : at + NBUF * (k + 1)] for k in range(NP)]
    wg, wu, wd, dgs, dus, send, recv, local = refs[at + NBUF * NP :]
    loads = lambda: [pltpu.make_async_copy(a, b, local.at[8 + n]) for n, (a, b) in enumerate(zip(hbm_w, (wg, wu, wd), strict=True))]

    j, i = pl.program_id(0), pl.program_id(1)
    step = j * TILES + i
    p = Place()
    z = p.z
    beside, across = z + 1 - 2 * (z % 2), 3 - z
    half_beside, half_across = (z + z // 2) % 2, z // 2

    @pl.when(step == 0)
    def _():
        barrier = pltpu.get_barrier_semaphore()
        for n in (p.partner, p.nx, p.ny, p.diag):
            signal(barrier, p.at(n))
        for n in range(1, 4):
            signal(barrier, p.at(p.s, lax.rem(z + n, 4)))
        pl.semaphore_wait(barrier, 7)
        for cp in loads():
            cp.start()

    def piece_stage(k, stage):
        r0, s1, r1, s2, r2, zs, zr, zt, zp, fin = bufs[k]
        one, two_, half = (beside, across, half_beside) if k % 2 == 0 else (across, beside, half_across)
        other = 1 - half
        x_first = k % 2 == 0
        mine, theirs = (p.x, p.x_) if x_first else (p.y, p.y_)
        mine_b, theirs_b = (p.y, p.y_) if x_first else (p.x, p.x_)
        na, nb = (p.nx, p.ny) if x_first else (p.ny, p.nx)

        def hop(n, src, dst, device):
            return copy_to(src, dst, send.at[k, n], recv.at[k, n], device)

        def chip(first, second):
            return (first, second) if x_first else (second, first)

        if k < 8:
            source = bulk[k // 2].at[:, :, p.c_, k % 2]
            own_half = lambda: pltpu.make_async_copy(bulk[k // 2].at[:, :, p.c, k % 2], bulk_own[k], local.at[k])
            term = lambda u, v: bulk_own[k][u, v].astype(F32)
            term_half = lambda u, v, h: bulk_own[k][u, v, h].astype(F32)
        else:
            source = chunk_g[k - 8].at[:, :, p.c_]
            own_half = None
            term = lambda u, v: chunk_g[k - 8][u, v, p.c].astype(F32)
            term_half = lambda u, v, h: chunk_g[k - 8][u, v, p.c, h].astype(F32)

        def two(first, second):
            u, v = chip(first, second)
            return term(u, v) + r0[u, v].astype(F32)

        cps = (
            lambda: hop(0, source, r0, p.at(p.partner)),
            lambda: hop(1, s1, r1, p.at(na)),
            lambda: hop(2, s2, r2, p.at(nb)),
        )
        def finish():
            for h in range(2):
                if k < 4:
                    lo = 32 * (k % 2) + 16 * h
                    (og, ou)[k // 2][1, lo : lo + 16, :] = fin[h]
                elif k < 8:
                    lo = 256 * (k % 2) + 128 * h
                    od[(7 - k) // 2, :, lo : lo + 128] = fin[h]
                else:
                    lo, n = CHUNKS[(k - 8) // 2]
                    (og, ou)[k % 2][0, 32 * h : 32 * h + 32, lo : lo + n] = fin[h]

        if k >= DIRECT:
            chips = ((p.x_, p.y), (p.x, p.y_), (p.x_, p.y_))
            across_chips = [
                lambda n=n, u=u, v=v: hop(1 + n, s1.at[n], r1.at[n], p.at(p.core(u, v, p.c)))
                for n, (u, v) in enumerate(chips)
            ]
            along = [
                lambda n=n: hop(4 + n, zs.at[z], zs.at[z], p.at(p.s, lax.rem(z + 1 + n, 4)))
                for n in range(3)
            ]
            arrived = [
                lambda n=n, q=lax.rem(z + 3 - n, 4): hop(4 + n, zs.at[q], zs.at[q], p.at(p.s, q))
                for n in range(3)
            ]
            if stage == 0:
                cps[0]().start()
            if stage == 1:
                cps[0]().wait_recv()
                for n in (2, 0, 1):
                    s1[n] = two(*chip(*chips[n])).astype(BF16)
                    across_chips[n]().start()
            if stage == 2:
                for cp in across_chips:
                    cp().wait_recv()
                total = two(*chip(p.x, p.y))
                for n in range(3):
                    total += r1[n].astype(F32)
                zs[z] = total.astype(BF16)
                for cp in along:
                    cp().start()
            if stage == 3:
                for cp in arrived:
                    cp().wait_recv()
                total = jnp.sum(zs[...].astype(F32), 0)
                fin[...] = total.astype(BF16)
                finish()
            if stage == 4:
                for cp in [cps[0]] + across_chips + along:
                    cp().wait_send()
            return

        if stage == 0:
            cps[0]().start()
            if own_half is not None:
                own_half().start()
        if stage == 1:
            cps[0]().wait_recv()
            if own_half is not None:
                own_half().wait()
            for q in range(2):
                s1[q] = two(theirs, q).astype(BF16)
            cps[1]().start()
        if stage == 2:
            cps[1]().wait_recv()
            s2[...] = (two(mine, theirs_b) + r1[theirs_b].astype(F32)).astype(BF16)
            cps[2]().start()
        z_cps = (
            lambda: hop(3, zs, zr, p.at(p.s, one)),
            lambda: hop(4, zt, zp, p.at(p.s, two_)),
            lambda: hop(5, fin.at[half], fin.at[half], p.at(p.s, one)),
        )

        def xy_sum(h):
            u, v = chip(mine, mine_b)
            return term_half(u, v, h) + r0[u, v, h].astype(F32) + r1[mine_b, h].astype(F32) + r2[h].astype(F32)

        if stage == 3:
            cps[2]().wait_recv()
            zs[...] = xy_sum(other).astype(BF16)
            z_cps[0]().start()
        if stage == 4:
            z_cps[0]().wait_recv()
            zt[...] = (xy_sum(half) + zr[...].astype(F32)).astype(BF16)
            z_cps[1]().start()
        if stage == 5:
            z_cps[1]().wait_recv()
            fin[half] = (zt[...].astype(F32) + zp[...].astype(F32)).astype(BF16)
            z_cps[2]().start()
        if stage == 6:
            hop(5, fin.at[other], fin.at[other], p.at(p.s, one)).wait_recv()
            for cp in z_cps:
                cp().wait_send()
            for cp in cps:
                cp().wait_send()
            finish()

    plan = schedule()

    def events(now):
        for when, stage, k in plan:
            if when == now:
                piece_stage(k, stage)

    for now in sorted({e[0] for e in plan if e[0] < STEPS}):
        pl.when(step == now)(functools.partial(events, now))

    @pl.when(step == 0)
    def _():
        for cp in loads():
            cp.wait()

    @pl.when(j == 0)
    def _():
        a_t[i] = a_ref[...].T

    def body(n, lo, first):
        a, dh = a_ref[...], dh_ref[...]
        for at, width in pieces_of(0, n):
            cut = pl.ds(lo + at, width)
            g = dot(a, wg[:, cut])
            u = dot(a, wu[:, cut])
            da = dot_nt(dh, wd[cut, :]).astype(BF16).astype(F32)
            sig, si = gated(g)
            dus[:, at : at + width] = (da * si).astype(BF16)
            dgs[:, at : at + width] = (da * u * (sig + si * (1.0 - sig))).astype(BF16)
        at_tile = a_t[i]
        pg, pu = dot(at_tile, dgs[:, :n]), dot(at_tile, dus[:, :n])

        @pl.when(i == 0)
        def _():
            accg[:, :n] = pg
            accu[:, :n] = pu

        @pl.when(i > 0)
        def _():
            accg[:, :n] += pg
            accu[:, :n] += pu

    @pl.when(j < 3)
    def _():
        body(512, pl.multiple_of(j * 512, 512), None)

    @pl.when(j == 3)
    def _():
        body(128, 1536, None)

    for k, (lo, n) in enumerate(CHUNKS):

        @pl.when((j == k) & (i == TILES - 1))
        def _(k=k, n=n):
            for acc, out in ((accg, chunk_g[2 * k]), (accu, chunk_g[2 * k + 1])):
                for q in range(16):
                    c_, h_ = (q // 2) % 2, q % 2
                    out[q // 8, (q // 4) % 2, c_, h_] = acc[32 * q : 32 * q + 32, :n].astype(BF16)

    pl.when(step == STEPS - 1)(functools.partial(events, STEPS))


def backward0(a0, dh1, w, bulk):
    tile2 = lambda n: pl.BlockSpec((TILE, n), lambda j, i: (i, 0))
    bufs = []
    for k, (hr, hc) in enumerate(PIECES):
        one, four = (hr, hc), (2, 2, hr, hc)
        if k < DIRECT:
            shapes = (2,) + four, four, four, (2,) + one, (2,) + one, one, one, one, one, (2,) + one
        else:
            shapes = (2,) + four, (3, 2) + one, (3, 2) + one, one, one, (4, 2) + one, one, one, one, (2,) + one
        bufs += [pltpu.VMEM(shape, BF16) for shape in shapes]
    up, down = jax.ShapeDtypeStruct((2, 64, FF), BF16), jax.ShapeDtypeStruct((2, 208, D), BF16)
    bulk = [t.reshape((2, 2, 2, 2, 2) + shape) for t, shape in zip(bulk, BULK[::2], strict=True)]
    return pl.pallas_call(
        backward0_kernel,
        grid=(len(CHUNKS), TILES),
        out_shape=[up, up, down],
        in_specs=[tile2(D), tile2(D)] + [ANY] * 7,
        out_specs=[WHOLE] * 3,
        scratch_shapes=[pltpu.VMEM((TILES, D, TILE), BF16)]
        + [pltpu.VMEM((D, 512), F32)] * 2
        + [pltpu.VMEM((2, 2, 2, 2, 32, n), BF16) for _, n in CHUNKS for _ in range(2)]
        + [pltpu.VMEM((2, 2, 2) + shape, BF16) for shape in BULK]
        + bufs
        + [pltpu.VMEM((D, FF), BF16), pltpu.VMEM((D, FF), BF16), pltpu.VMEM((FF, D), BF16)]
        + [pltpu.VMEM((TILE, 512), BF16)] * 2
        + [pltpu.SemaphoreType.DMA((NP, 7)), pltpu.SemaphoreType.DMA((NP, 7)), pltpu.SemaphoreType.DMA((11,))],
        compiler_params=pltpu.CompilerParams(
            collective_id=1, has_side_effects=True, vmem_limit_bytes=VMEM_LIMIT, dimension_semantics=("arbitrary", "arbitrary")
        ),
        name="backward0",
    )(a0, dh1, *w, *bulk)


def adamw(w, m, v, g):
    m = 0.9 * m + 0.1 * g
    v = 0.95 * v + 0.05 * g * g
    step = m * lax.rsqrt(v + 1e-8) + 0.1 * w
    return (w - 0.02 * step).astype(BF16), m, v


def solution(mesh):
    def step(x, dy, *arrays):
        weights, m, v = (arrays[i : i + 3] for i in (0, 3, 6))
        h1, act0, a0, w0, w1 = forward(x[0], weights)
        dh1, *bulk = layer1(h1, dy[0], act0, w1)
        gradients = backward0(a0, dh1, w0, bulk)
        new = [adamw(w.astype(F32), m, v, g.astype(F32)) for w, m, v, g in zip(weights, m, v, gradients, strict=True)]
        return tuple(one[which] for which in range(3) for one in new)

    states, cut = P(("rep", "r", "s"), None, None), P(None, "s", None)
    return jax.shard_map(
        step,
        mesh=mesh,
        in_specs=(states, states) + (cut,) * 9,
        out_specs=(P("rep", "s", None),) * 9,
        check_vma=False,
    )
```

```python
import functools

import jax
import jax.numpy as jnp
from jax import lax
from jax.experimental import pallas as pl
from jax.experimental.pallas import tpu as pltpu
from jax.sharding import PartitionSpec as P

F32, BF16 = jnp.float32, jnp.bfloat16
D, FF, TOK = 512, 1664, 4096
TILE = 1024
STRIP = 256
TILES = TOK // TILE
CHUNKS = ((0, 512), (512, 512), (1024, 512), (1536, 128))
VMEM_LIMIT = 66_000_000
ANY = pl.BlockSpec(memory_space=pl.ANY)
WHOLE = pl.BlockSpec(memory_space=pltpu.VMEM)


def pieces_of(lo, n):
    return [(lo + at, min(STRIP, n - at)) for at in range(0, n, STRIP)]


def dot(a, b):
    return jnp.dot(a, b, preferred_element_type=F32)


def dot_nt(a, b):
    return lax.dot_general(a, b, (((1,), (1,)), ((), ())), preferred_element_type=F32)


def norm(h):
    wide = h.astype(F32)
    scale = lax.rsqrt(jnp.mean(wide * wide, -1, keepdims=True) + 1e-6)
    return wide, scale


def gated(g):
    sig = 0.5 + 0.5 * jnp.tanh(0.5 * g)
    return sig, g * sig


def rows(n):
    return pl.BlockSpec((TILE, n), lambda i: (i, 0))


class Place:
    def __init__(self):
        s, z = lax.axis_index("s"), lax.axis_index("r")
        self.s, self.z = s, z
        self.x, self.y, self.c = s // 4, (s // 2) % 2, s % 2
        x, y, c = self.x, self.y, self.c
        self.x_, self.y_, self.c_ = 1 - x, 1 - y, 1 - c
        self.partner = self.core(x, y, self.c_)
        self.nx = self.core(self.x_, y, c)
        self.ny = self.core(x, self.y_, c)
        self.diag = self.core(self.x_, self.y_, c)

    @staticmethod
    def core(x, y, c):
        return x * 4 + y * 2 + c

    def at(self, s, z=None):
        return (0, self.z if z is None else z, s)


def copy_to(src, dst, send, recv, device):
    return pltpu.make_async_remote_copy(
        src_ref=src, dst_ref=dst, send_sem=send, recv_sem=recv, device_id=device, device_id_type=pl.DeviceIdType.MESH
    )


def signal(barrier, device):
    pl.semaphore_signal(barrier, inc=1, device_id=device, device_id_type=pl.DeviceIdType.MESH)


EARLY = 768
GATHERED = tuple((m, 0, lo, n) for lo, n in ((0, EARLY), (EARLY, FF - EARLY)) for m in (0, 1)) + ((2, 0, 0, D),)
GATHERED += tuple((m, 1, 0, n) for m, n in enumerate((FF, FF, D)))
NG = len(GATHERED)
FORWARD_STEPS = 3 * TILES
OWN, PASS, DIAG, DONE = range(4)
GATHER_PLAN = {
    0: ((OWN, 0, 1, 2), (PASS, 0, 1), (OWN, 3), (DIAG, 0, 1), (DONE, 0, 1), (PASS, 2)),
    1: ((PASS, 3), (OWN, 4, 5)),
    4: ((DIAG, 2, 3), (DONE, 2, 3), (OWN, 6)),
    5: ((PASS, 4), (OWN, 7)),
    6: ((PASS, 5),),
    7: ((PASS, 6),),
    8: ((DIAG, 4), (DONE, 4)),
    9: ((PASS, 7),),
    10: ((DIAG, 5),),
    11: ((DIAG, 6),),
    12: ((DIAG, 7), (DONE, 5, 6, 7)),
}


def forward_kernel(og, ou, od, x_ref, h1_ref, act_ref, a_ref, *refs):
    keep, later = refs[:3], refs[3:6]
    w0 = refs[6:9]
    acts, norms = refs[9:11]
    send, recv, local = refs[11:14]
    own = (og, ou, od)
    step = pl.program_id(0)
    p = Place()

    def block(i, slot):
        m, layer, lo, n = GATHERED[i]
        return (later if layer else w0)[m].at[slot, :, pl.ds(lo, n)]

    def cp(i, k):
        m, layer, lo, n = GATHERED[i]
        mine = own[m].at[layer, :, pl.ds(lo, n)]
        src, slot, device = (
            (mine, p.s, p.nx),
            (mine, p.s, p.ny),
            (mine, p.s, p.partner),
            (block(i, p.nx), p.nx, p.partner),
            (block(i, p.ny), p.ny, p.partner),
            (block(i, p.nx), p.nx, p.ny) if i % 2 == 0 else (block(i, p.ny), p.ny, p.nx),
            (block(i, p.diag), p.diag, p.partner),
        )[k]
        return copy_to(src, block(i, slot), send.at[i, k], recv.at[i, k], p.at(device))

    def do(what, i):
        if what == OWN:
            for k in range(3):
                cp(i, k).start()
        elif what == PASS:
            first, then = (0, 1) if i % 2 == 0 else (1, 0)
            cp(i, first).wait_recv()
            cp(i, 5).start()
            cp(i, 3 + first).start()
            cp(i, then).wait_recv()
            cp(i, 3 + then).start()
        elif what == DIAG:
            cp(i, 5).wait_recv()
            cp(i, 6).start()
        else:
            for k in (2, 3, 4, 6):
                cp(i, k).wait_recv()

    def follow(now):
        for what, *items in GATHER_PLAN[now]:
            for i in items:
                do(what, i)

    def own_out(m):
        return pltpu.make_async_copy(own[m].at[1], later[m].at[p.s], local.at[m])

    def w0_out(m):
        return pltpu.make_async_copy(w0[m], keep[m], local.at[3 + m])

    def act_out(t):
        return pltpu.make_async_copy(acts.at[t], act_ref.at[pl.ds(t * TILE, TILE)], local.at[6 + t])

    def norm_out(t):
        return pltpu.make_async_copy(norms.at[t], a_ref.at[pl.ds(t * TILE, TILE)], local.at[6 + TILES + t])

    @pl.when(step == 0)
    def _():
        barrier = pltpu.get_barrier_semaphore()
        for n in (p.partner, p.nx, p.ny):
            signal(barrier, p.at(n))
        pl.semaphore_wait(barrier, 3)
        for m in range(3):
            w0[m][p.s] = own[m][0]
            own_out(m).start()

    @pl.when(step < TILES)
    def _():
        wide, scale = norm(x_ref[...])
        norms[step] = (wide * scale).astype(BF16)

    for now in GATHER_PLAN:
        if now < FORWARD_STEPS:
            pl.when(step == now)(functools.partial(follow, now))

    def up(t, lo, n):
        for at, width in pieces_of(lo, n):
            cut = slice(at, at + width)
            g = dot(norms[t], w0[0][:, :, cut].reshape(D, width))
            u = dot(norms[t], w0[1][:, :, cut].reshape(D, width))
            acts[t, :, cut] = (gated(g)[1] * u).astype(BF16)

    @pl.when(step < TILES)
    def _():
        up(step, 0, EARLY)

    @pl.when((step >= TILES) & (step < 2 * TILES))
    def _():
        up(step - TILES, EARLY, FF - EARLY)

    @pl.when(step >= 2 * TILES)
    def _():
        mm = dot(acts[step - 2 * TILES], w0[2][...].reshape(FF, D)).astype(BF16).astype(F32)
        h1_ref[...] = (x_ref[...].astype(F32) + mm).astype(BF16)

    for k in range(TILES):

        @pl.when(step == TILES + 1 + k)
        def _(k=k):
            act_out(k).start()
            norm_out(k).start()

    @pl.when(step == 2 * TILES + 1)
    def _():
        for m in range(3):
            w0_out(m).start()

    @pl.when(step == FORWARD_STEPS - 1)
    def _():
        follow(FORWARD_STEPS)
        for i in range(NG):
            for k in range(7):
                cp(i, k).wait_send()
        for m in range(3):
            own_out(m).wait()
            w0_out(m).wait()
        for k in range(TILES):
            act_out(k).wait()
            norm_out(k).wait()


def forward(x, weights):
    blocks = [jax.ShapeDtypeStruct((8,) + w.shape[1:], BF16) for w in weights]
    h1, act, a, *full = pl.pallas_call(
        forward_kernel,
        grid=(FORWARD_STEPS,),
        out_shape=[
            jax.ShapeDtypeStruct((TOK, D), BF16),
            jax.ShapeDtypeStruct((TOK, FF), BF16),
            jax.ShapeDtypeStruct((TOK, D), BF16),
        ]
        + blocks * 2,
        in_specs=[WHOLE, WHOLE, WHOLE, pl.BlockSpec((TILE, D), lambda n: (jnp.where(n < TILES, n, jnp.maximum(n - 2 * TILES, 0)), 0))],
        out_specs=[pl.BlockSpec((TILE, D), lambda n: (jnp.maximum(n - 2 * TILES, 0), 0))] + [ANY] * 8,
        scratch_shapes=[pltpu.VMEM(b.shape, BF16) for b in blocks]
        + [pltpu.VMEM((TILES, TILE, FF), BF16), pltpu.VMEM((TILES, TILE, D), BF16)]
        + [pltpu.SemaphoreType.DMA((NG, 7)), pltpu.SemaphoreType.DMA((NG, 7)), pltpu.SemaphoreType.DMA((6 + 2 * TILES,))],
        compiler_params=pltpu.CompilerParams(
            collective_id=0, has_side_effects=True, vmem_limit_bytes=VMEM_LIMIT, dimension_semantics=("arbitrary",)
        ),
        name="forward",
    )(*weights, x)
    full = [o.reshape(8 * o.shape[1], o.shape[2]) for o in full]
    return h1, act, a, full[:3], full[3:]


def layer1_kernel(h_ref, dy_ref, act0_ref, wg, wu, wd, dh_ref, og, ou, od, od0, accg, accu, accd, accd0, dgs, dus, acts):
    i = pl.program_id(0)

    @pl.when(i == 0)
    def _():
        for acc in (accg, accu, accd, accd0):
            acc[...] = jnp.zeros_like(acc)

    wide, scale = norm(h_ref[...])
    a = (wide * scale).astype(BF16)
    a_t = a.T
    dy = dy_ref[...]
    dy_t = dy.T
    for lo, n in pieces_of(0, FF):
        cut = slice(lo, lo + n)
        g = dot(a, wg[:, cut])
        u = dot(a, wu[:, cut])
        da = dot_nt(dy, wd[cut, :]).astype(BF16).astype(F32)
        sig, si = gated(g)
        act = (si * u).astype(BF16)
        du = (da * si).astype(BF16)
        dg = (da * u * (sig + si * (1.0 - sig))).astype(BF16)
        dgs[:, cut] = dg
        dus[:, cut] = du
        acts[:, cut] = act
    accd[...] += dot(dy_t, acts[...])
    accg[...] += dot(a_t, dgs[...])
    accu[...] += dot(a_t, dus[...])
    dn = (dot_nt(dgs[...], wg[...]) + dot_nt(dus[...], wu[...])).astype(BF16).astype(F32)
    inner = jnp.sum(dn * wide, -1, keepdims=True) * (scale * scale * scale * (1.0 / D))
    by_norm = (dn * scale - wide * inner).astype(BF16).astype(F32)
    dh = (dy.astype(F32) + by_norm).astype(BF16)
    dh_ref[...] = dh
    accd0[...] += dot(dh.T, act0_ref[...])

    @pl.when(i == TILES - 1)
    def _():
        og[...] = accg[...].astype(BF16)
        ou[...] = accu[...].astype(BF16)
        for acc, out in ((accd, od), (accd0, od0)):
            for h in range(4):
                t = acc[128 * h : 128 * h + 128, :].T.astype(BF16)
                for s in range(8):
                    out[s, h] = t[208 * s : 208 * s + 208]


def layer1(h1, dy, act0, w):
    up, down = jax.ShapeDtypeStruct((D, FF), BF16), jax.ShapeDtypeStruct((8, 4, 208, 128), BF16)
    return pl.pallas_call(
        layer1_kernel,
        grid=(TILES,),
        out_shape=[jax.ShapeDtypeStruct((TOK, D), BF16), up, up, down, down],
        in_specs=[rows(D), rows(D), rows(FF), WHOLE, WHOLE, WHOLE],
        out_specs=[rows(D), WHOLE, WHOLE, WHOLE, WHOLE],
        scratch_shapes=[pltpu.VMEM((D, FF), F32)] * 4 + [pltpu.VMEM((TILE, FF), BF16)] * 3,
        compiler_params=pltpu.CompilerParams(vmem_limit_bytes=VMEM_LIMIT, dimension_semantics=("arbitrary",)),
        name="layer1",
    )(h1, dy, act0, *w)


BULK = ((16, FF),) * 4 + ((208, 128),) * 4
PIECES = BULK + tuple((32, n) for _, n in CHUNKS for _ in range(2))
NP = len(PIECES)
NBUF = 10
DIRECT = NP - 2


def schedule():
    plan = []

    def put(pair, *steps):
        for piece in (pair, pair + 1):
            for stage in range(STAGES):
                plan.append((steps[stage] if stage < len(steps) else STEPS, stage, piece))

    put(0, 0, 0, 2, 4, 6, 8)
    put(2, 0, 1, 3, 6, 8, 10)
    put(4, 0, 2, 5, 8, 11, 13)
    put(6, 0, 3, 7, 9, 12, 14)
    put(8, 4, 5, 8, 10, 13, 15)
    put(10, 8, 9, 11, 13, 15)
    put(12, 12, 13, 15)
    put(14)
    def rank(e):
        step, stage, piece = e
        if step == STEPS:
            return (step, (stage if stage < 2 else 4 * stage - 1) if piece >= DIRECT else 2 * stage, piece)
        return (step, stage, piece) if step == 0 else (step, piece // 2, stage, piece)

    return sorted(plan, key=rank)


STAGES = 7
STEPS = len(CHUNKS) * TILES


def backward0_kernel(*refs):
    a_ref, dh_ref = refs[:2]
    hbm_w = refs[2:5]
    bulk = refs[5:9]
    og, ou, od = refs[9:12]
    a_t, accg, accu = refs[12:15]
    chunk_g = refs[15 : 15 + 2 * len(CHUNKS)]
    at = 15 + 2 * len(CHUNKS)
    bulk_own = refs[at : at + 8]
    at += 8
    bufs = [refs[at + NBUF * k : at + NBUF * (k + 1)] for k in range(NP)]
    wg, wu, wd, dgs, dus, send, recv, local = refs[at + NBUF * NP :]
    loads = lambda: [pltpu.make_async_copy(a, b, local.at[8 + n]) for n, (a, b) in enumerate(zip(hbm_w, (wg, wu, wd), strict=True))]

    j, i = pl.program_id(0), pl.program_id(1)
    step = j * TILES + i
    p = Place()
    z = p.z
    beside, across = z + 1 - 2 * (z % 2), 3 - z
    half_beside, half_across = (z + z // 2) % 2, z // 2

    @pl.when(step == 0)
    def _():
        barrier = pltpu.get_barrier_semaphore()
        for n in (p.partner, p.nx, p.ny, p.diag):
            signal(barrier, p.at(n))
        for n in range(1, 4):
            signal(barrier, p.at(p.s, lax.rem(z + n, 4)))
        pl.semaphore_wait(barrier, 7)
        for cp in loads():
            cp.start()

    def piece_stage(k, stage):
        r0, s1, r1, s2, r2, zs, zr, zt, zp, fin = bufs[k]
        one, two_, half = (beside, across, half_beside) if k % 2 == 0 else (across, beside, half_across)
        other = 1 - half
        x_first = k % 2 == 0
        mine, theirs = (p.x, p.x_) if x_first else (p.y, p.y_)
        mine_b, theirs_b = (p.y, p.y_) if x_first else (p.x, p.x_)
        na, nb = (p.nx, p.ny) if x_first else (p.ny, p.nx)

        def hop(n, src, dst, device):
            return copy_to(src, dst, send.at[k, n], recv.at[k, n], device)

        def chip(first, second):
            return (first, second) if x_first else (second, first)

        if k < 8:
            source = bulk[k // 2].at[:, :, p.c_, k % 2]
            own_half = lambda: pltpu.make_async_copy(bulk[k // 2].at[:, :, p.c, k % 2], bulk_own[k], local.at[k])
            term = lambda u, v: bulk_own[k][u, v].astype(F32)
            term_half = lambda u, v, h: bulk_own[k][u, v, h].astype(F32)
        else:
            source = chunk_g[k - 8].at[:, :, p.c_]
            own_half = None
            term = lambda u, v: chunk_g[k - 8][u, v, p.c].astype(F32)
            term_half = lambda u, v, h: chunk_g[k - 8][u, v, p.c, h].astype(F32)

        def two(first, second):
            u, v = chip(first, second)
            return term(u, v) + r0[u, v].astype(F32)

        cps = (
            lambda: hop(0, source, r0, p.at(p.partner)),
            lambda: hop(1, s1, r1, p.at(na)),
            lambda: hop(2, s2, r2, p.at(nb)),
        )
        def finish():
            for h in range(2):
                if k < 4:
                    lo = 32 * (k % 2) + 16 * h
                    (og, ou)[k // 2][1, lo : lo + 16, :] = fin[h]
                elif k < 8:
                    lo = 256 * (k % 2) + 128 * h
                    od[(7 - k) // 2, :, lo : lo + 128] = fin[h]
                else:
                    lo, n = CHUNKS[(k - 8) // 2]
                    (og, ou)[k % 2][0, 32 * h : 32 * h + 32, lo : lo + n] = fin[h]

        if k >= DIRECT:
            chips = ((p.x_, p.y), (p.x, p.y_), (p.x_, p.y_))
            across_chips = [
                lambda n=n, u=u, v=v: hop(1 + n, s1.at[n], r1.at[n], p.at(p.core(u, v, p.c)))
                for n, (u, v) in enumerate(chips)
            ]
            along = [
                lambda n=n: hop(4 + n, zs.at[z], zs.at[z], p.at(p.s, lax.rem(z + 1 + n, 4)))
                for n in range(3)
            ]
            arrived = [
                lambda n=n, q=lax.rem(z + 3 - n, 4): hop(4 + n, zs.at[q], zs.at[q], p.at(p.s, q))
                for n in range(3)
            ]
            if stage == 0:
                cps[0]().start()
            if stage == 1:
                cps[0]().wait_recv()
                for n in (2, 0, 1):
                    s1[n] = two(*chip(*chips[n])).astype(BF16)
                    across_chips[n]().start()
            if stage == 2:
                for cp in across_chips:
                    cp().wait_recv()
                total = two(*chip(p.x, p.y))
                for n in range(3):
                    total += r1[n].astype(F32)
                zs[z] = total.astype(BF16)
                for cp in along:
                    cp().start()
            if stage == 3:
                for cp in arrived:
                    cp().wait_recv()
                total = jnp.sum(zs[...].astype(F32), 0)
                fin[...] = total.astype(BF16)
                finish()
            if stage == 4:
                for cp in [cps[0]] + across_chips + along:
                    cp().wait_send()
            return

        if stage == 0:
            cps[0]().start()
            if own_half is not None:
                own_half().start()
        if stage == 1:
            cps[0]().wait_recv()
            if own_half is not None:
                own_half().wait()
            for q in range(2):
                s1[q] = two(theirs, q).astype(BF16)
            cps[1]().start()
        if stage == 2:
            cps[1]().wait_recv()
            s2[...] = (two(mine, theirs_b) + r1[theirs_b].astype(F32)).astype(BF16)
            cps[2]().start()
        z_cps = (
            lambda: hop(3, zs, zr, p.at(p.s, one)),
            lambda: hop(4, zt, zp, p.at(p.s, two_)),
            lambda: hop(5, fin.at[half], fin.at[half], p.at(p.s, one)),
        )

        def xy_sum(h):
            u, v = chip(mine, mine_b)
            return term_half(u, v, h) + r0[u, v, h].astype(F32) + r1[mine_b, h].astype(F32) + r2[h].astype(F32)

        if stage == 3:
            cps[2]().wait_recv()
            zs[...] = xy_sum(other).astype(BF16)
            z_cps[0]().start()
        if stage == 4:
            z_cps[0]().wait_recv()
            zt[...] = (xy_sum(half) + zr[...].astype(F32)).astype(BF16)
            z_cps[1]().start()
        if stage == 5:
            z_cps[1]().wait_recv()
            fin[half] = (zt[...].astype(F32) + zp[...].astype(F32)).astype(BF16)
            z_cps[2]().start()
        if stage == 6:
            hop(5, fin.at[other], fin.at[other], p.at(p.s, one)).wait_recv()
            for cp in z_cps:
                cp().wait_send()
            for cp in cps:
                cp().wait_send()
            finish()

    plan = schedule()

    def events(now):
        for when, stage, k in plan:
            if when == now:
                piece_stage(k, stage)

    for now in sorted({e[0] for e in plan if e[0] < STEPS}):
        pl.when(step == now)(functools.partial(events, now))

    @pl.when(step == 0)
    def _():
        for cp in loads():
            cp.wait()

    @pl.when(j == 0)
    def _():
        a_t[i] = a_ref[...].T

    def body(n, lo, first):
        a, dh = a_ref[...], dh_ref[...]
        for at, width in pieces_of(0, n):
            cut = pl.ds(lo + at, width)
            g = dot(a, wg[:, cut])
            u = dot(a, wu[:, cut])
            da = dot_nt(dh, wd[cut, :]).astype(BF16).astype(F32)
            sig, si = gated(g)
            dus[:, at : at + width] = (da * si).astype(BF16)
            dgs[:, at : at + width] = (da * u * (sig + si * (1.0 - sig))).astype(BF16)
        at_tile = a_t[i]
        pg, pu = dot(at_tile, dgs[:, :n]), dot(at_tile, dus[:, :n])

        @pl.when(i == 0)
        def _():
            accg[:, :n] = pg
            accu[:, :n] = pu

        @pl.when(i > 0)
        def _():
            accg[:, :n] += pg
            accu[:, :n] += pu

    @pl.when(j < 3)
    def _():
        body(512, pl.multiple_of(j * 512, 512), None)

    @pl.when(j == 3)
    def _():
        body(128, 1536, None)

    for k, (lo, n) in enumerate(CHUNKS):

        @pl.when((j == k) & (i == TILES - 1))
        def _(k=k, n=n):
            for acc, out in ((accg, chunk_g[2 * k]), (accu, chunk_g[2 * k + 1])):
                for q in range(16):
                    c_, h_ = (q // 2) % 2, q % 2
                    out[q // 8, (q // 4) % 2, c_, h_] = acc[32 * q : 32 * q + 32, :n].astype(BF16)

    pl.when(step == STEPS - 1)(functools.partial(events, STEPS))


def backward0(a0, dh1, w, bulk):
    tile2 = lambda n: pl.BlockSpec((TILE, n), lambda j, i: (i, 0))
    bufs = []
    for k, (hr, hc) in enumerate(PIECES):
        one, four = (hr, hc), (2, 2, hr, hc)
        if k < DIRECT:
            shapes = (2,) + four, four, four, (2,) + one, (2,) + one, one, one, one, one, (2,) + one
        else:
            shapes = (2,) + four, (3, 2) + one, (3, 2) + one, one, one, (4, 2) + one, one, one, one, (2,) + one
        bufs += [pltpu.VMEM(shape, BF16) for shape in shapes]
    up, down = jax.ShapeDtypeStruct((2, 64, FF), BF16), jax.ShapeDtypeStruct((2, 208, D), BF16)
    bulk = [t.reshape((2, 2, 2, 2, 2) + shape) for t, shape in zip(bulk, BULK[::2], strict=True)]
    return pl.pallas_call(
        backward0_kernel,
        grid=(len(CHUNKS), TILES),
        out_shape=[up, up, down],
        in_specs=[tile2(D), tile2(D)] + [ANY] * 7,
        out_specs=[WHOLE] * 3,
        scratch_shapes=[pltpu.VMEM((TILES, D, TILE), BF16)]
        + [pltpu.VMEM((D, 512), F32)] * 2
        + [pltpu.VMEM((2, 2, 2, 2, 32, n), BF16) for _, n in CHUNKS for _ in range(2)]
        + [pltpu.VMEM((2, 2, 2) + shape, BF16) for shape in BULK]
        + bufs
        + [pltpu.VMEM((D, FF), BF16), pltpu.VMEM((D, FF), BF16), pltpu.VMEM((FF, D), BF16)]
        + [pltpu.VMEM((TILE, 512), BF16)] * 2
        + [pltpu.SemaphoreType.DMA((NP, 7)), pltpu.SemaphoreType.DMA((NP, 7)), pltpu.SemaphoreType.DMA((11,))],
        compiler_params=pltpu.CompilerParams(
            collective_id=1, has_side_effects=True, vmem_limit_bytes=VMEM_LIMIT, dimension_semantics=("arbitrary", "arbitrary")
        ),
        name="backward0",
    )(a0, dh1, *w, *bulk)


def adamw(w, m, v, g):
    m = 0.9 * m + 0.1 * g
    v = 0.95 * v + 0.05 * g * g
    step = m * lax.rsqrt(v + 1e-8) + 0.1 * w
    return (w - 0.02 * step).astype(BF16), m, v


def solution(mesh):
    def step(x, dy, *arrays):
        weights, m, v = (arrays[i : i + 3] for i in (0, 3, 6))
        h1, act0, a0, w0, w1 = forward(x[0], weights)
        dh1, *bulk = layer1(h1, dy[0], act0, w1)
        gradients = backward0(a0, dh1, w0, bulk)
        new = [adamw(w.astype(F32), m, v, g.astype(F32)) for w, m, v, g in zip(weights, m, v, gradients, strict=True)]
        return tuple(one[which] for which in range(3) for one in new)

    states, cut = P(("rep", "r", "s"), None, None), P(None, "s", None)
    return jax.shard_map(
        step,
        mesh=mesh,
        in_specs=(states, states) + (cut,) * 9,
        out_specs=(P("rep", "s", None),) * 9,
        check_vma=False,
    )
```
